32 devices in a mesh: seq: 8 (over z, x), tp: 4 (over y, core).
Axes of the slice: x: 2, y: 2, z: 4, core: 2. Of those that a mesh axis runs over, the one named last changes fastest.
Arguments:
- queries: bfloat16 [1536, 6144], P('seq', 'tp'), may hold values from -400 to 400
- key_vectors: bfloat16 [1536, 1024], P('seq', 'tp'), may hold values from -8 to 8
- value_vectors: bfloat16 [1536, 1024], P('seq', 'tp'), may hold values from -6 to 6
- positions: int32 [1536], P('seq'), may hold values from 0 to 1535, as said below
- residual: bfloat16 [1536, 6144], P('seq', 'tp'), may hold values from -200 to 200
- norm_gain: float32 [1, 6144], P(None, 'tp'), may hold values from 0.5 to 1.5
- out_weight: bfloat16 [6144, 6144], P('tp'), may hold values from -0.3125 to 0.3125
Outputs:
- quantized: bfloat16 [1536, 6144], P('seq')
- token_scale: float32 [1536], P('seq')
- new_residual: bfloat16 [1536, 6144], P('seq', 'tp')
The draws below stay inside these ranges and needn't reach their ends.
Inputs may be any that keep to these rules, and one draw needn't show every extreme that they name: The positions are a permutation of 0 to 1535. Cut into 16 runs of 96 consecutive positions, the rows of one index of seq hold run r in their first 96 rows and run 2 * 8 - 1 - r in their last ones, both in increasing order, with r differing between the indices of seq.
All inputs are finite; a program needn't handle non-finite values. Where the reference program divides by a largest or mean magnitude, that divisor is 1e-20 or more.
Results may differ from the reference program's by a relative error of at most 0.012.
Values may be sent and summed in bfloat16 or wider, within the bound.
No kernel may reach another device: no remote copies, remote signals or barrier semaphores. Data moves between devices by JAX's collectives and lax.ppermute only.
A program may use at most 64 MiB of HBM per device.

```python
import math
import jax
import jax.numpy as jnp
from jax import lax

D = 6144
Q_HEADS = 48
KV_HEADS = 8
HEAD = 128
TOK_DEV = 192
TOKENS = 1536
N_SEQ = 8
N_TP = 4


def shared_keys(key):
    inner_key = jax.random.fold_in(key, 21)
    shape = (TOKENS, KV_HEADS * HEAD)
    base_draw = jax.random.truncated_normal(inner_key, -5.0, 5.0, shape, jnp.float32)
    return base_draw


def draw_key_vectors(key, part):
    base_draw = shared_keys(key)
    return base_draw.astype(jnp.bfloat16)


def draw_queries(key, part):
    shape = (TOKENS, Q_HEADS * HEAD)
    noise_key = jax.random.fold_in(key, 23)
    base_draw = 2.0 * jax.random.truncated_normal(noise_key, -5.0, 5.0, shape, jnp.float32)
    return base_draw.astype(jnp.bfloat16)


def draw_positions(key, part):
    run_order = jax.random.permutation(jax.random.fold_in(key, 11), N_SEQ).astype(jnp.int32)
    half_rows = TOK_DEV // 2
    lane_index = jnp.arange(half_rows, dtype=jnp.int32)
    first_run = run_order[:, None] * half_rows + lane_index[None, :]
    second = (2 * N_SEQ - 1 - run_order)[:, None] * half_rows + lane_index[None, :]
    return jnp.concatenate([first_run, second], axis=1).reshape(TOKENS).astype(jnp.int32)


def draw_residual(key, part):
    noise_key = jax.random.fold_in(key, 31)
    column_key = jax.random.fold_in(key, 32)
    row_key = jax.random.fold_in(key, 33)
    column_index = jnp.arange(D, dtype=jnp.float32)
    column_scale = 3.0 ** (column_index / D) * jnp.exp(jax.random.uniform(column_key, (D,), jnp.float32, 0.0, 1.2))
    noise = jax.random.truncated_normal(noise_key, -5.0, 5.0, (TOKENS, D), jnp.float32)
    row_scale = jnp.exp(jax.random.uniform(row_key, (TOKENS, 1), jnp.float32, 0.0, math.log(10.0)))
    return (0.2 * noise * row_scale * column_scale[None, :]).astype(jnp.bfloat16)


def steps_of(stream_key, extent, shards, low, largest):
    gain, own = 1.0, jax.random.fold_in(stream_key, 6)
    for position, shards_of in shards:
        draws = jnp.exp(jax.random.uniform(jax.random.fold_in(own, position), (shards_of,), jnp.float32, low / len(shards), largest / len(shards)))
        gain = gain * jnp.repeat(draws, extent[position] // shards_of).reshape([-1 if axis == position else 1 for axis in range(len(extent))])
    return gain


def centred(stream_key, extent, scale, reach, shards=(), kind=jnp.bfloat16):
    loudness = steps_of(stream_key, extent, shards, -0.22, 0.18) if shards else 1.0
    values = jax.random.normal(stream_key, extent, jnp.float32) * scale * loudness
    return jnp.minimum(jnp.maximum(values, -reach), reach).astype(kind)


def setup_inputs(seed: int = 0) -> dict:
    splits = jax.random.split(jax.random.key(seed), 8)
    return {
        "queries": draw_queries(jax.random.fold_in(splits[7], 71), 0),
        "key_vectors": draw_key_vectors(jax.random.fold_in(splits[7], 71), 0),
        "value_vectors": centred(splits[2], (TOKENS, KV_HEADS * HEAD), 1.0, 6.0, ((0, 8), (1, 4))),
        "positions": draw_positions(jax.random.fold_in(splits[7], 71), 0),
        "residual": draw_residual(jax.random.fold_in(splits[7], 71), 0),
        "norm_gain": jnp.clip(1.0 + 0.1 * jax.random.normal(splits[5], (1, D), jnp.float32), 0.5, 1.5),
        "out_weight": centred(splits[6], (Q_HEADS * HEAD, D), (Q_HEADS * HEAD // 16) ** -0.5, 0.3125, ((0, 4),)),
    }


def reference(queries, key_vectors, value_vectors, positions, residual, norm_gain, out_weight):
    token_count = queries.shape[0]
    group_size = Q_HEADS // KV_HEADS
    score_scale = 1.0 / math.sqrt(HEAD)
    query_heads = queries.reshape(token_count, Q_HEADS, HEAD).transpose(1, 0, 2)
    key_heads = key_vectors.reshape(token_count, KV_HEADS, HEAD).transpose(1, 0, 2)
    value_heads = value_vectors.reshape(token_count, KV_HEADS, HEAD).transpose(1, 0, 2)
    block_rows = TOK_DEV
    block_count = token_count // block_rows
    query_blocks = query_heads.reshape(Q_HEADS, block_count, block_rows, HEAD)
    pos_blocks = positions.reshape(block_count, block_rows)

    def one_head(head_index):
        key_rows = key_heads[head_index // group_size]
        value_rows = value_heads[head_index // group_size]

        def one_block(block_pair):
            query_block, block_pos = block_pair
            scores = jnp.dot(query_block, key_rows.T, preferred_element_type=jnp.float32) * score_scale
            visible = positions[None, :] <= block_pos[:, None]
            scores = jnp.where(visible, scores, -1e+30)
            row_max = lax.optimization_barrier(jnp.max(scores, axis=1, keepdims=True))
            raw_weights = jnp.where(visible, jnp.exp(scores - row_max), 0.0)
            weight_sum = lax.optimization_barrier(jnp.sum(raw_weights, axis=1, keepdims=True))
            mixed = jnp.dot(raw_weights.astype(jnp.bfloat16), value_rows, preferred_element_type=jnp.float32)
            return (mixed / weight_sum).astype(jnp.bfloat16)
        return lax.map(one_block, (query_blocks[head_index], pos_blocks))
    attended = lax.map(one_head, jnp.arange(Q_HEADS, dtype=jnp.int32))
    attended = attended.reshape(Q_HEADS, token_count, HEAD).transpose(1, 0, 2).reshape(token_count, Q_HEADS * HEAD)
    group_width = Q_HEADS * HEAD // N_TP
    summed = residual.astype(jnp.float32)
    for group_index in range(N_TP):
        lower = group_index * group_width
        partial_value = jnp.dot(attended[:, lower:lower + group_width], out_weight[lower:lower + group_width], preferred_element_type=jnp.float32)
        partial_value = lax.optimization_barrier(partial_value.astype(jnp.bfloat16))
        summed = summed + partial_value.astype(jnp.float32)
    new_residual = summed.astype(jnp.bfloat16)
    mean_square = lax.optimization_barrier(jnp.mean(summed * summed, axis=1, keepdims=True))
    normed = summed * lax.rsqrt(mean_square + 1e-05) * norm_gain
    token_scale = lax.optimization_barrier(jnp.max(jnp.abs(normed), axis=1)) + 1e-06
    quantized = (normed / token_scale[:, None]).astype(jnp.bfloat16)
    return (quantized, token_scale, new_residual)
```

```python
import functools
import math

import jax
import jax.numpy as jnp
from jax import lax
from jax.experimental import pallas as pl
from jax.experimental.pallas import tpu as pltpu
from jax.sharding import PartitionSpec as P

HEAD = 128
TAG_ROWS = 16
HIDE = -1e30
VMEM = pltpu.VMEM
F32 = jnp.float32
BF16 = jnp.bfloat16


def in_vmem():
    return pl.BlockSpec(memory_space=VMEM)


def in_smem():
    return pl.BlockSpec(memory_space=pltpu.SMEM)


def cost(flops, moved):
    return pl.CostEstimate(flops=int(flops), bytes_accessed=int(moved), transcendentals=0)


def pack_body(run_rows, pos_ref, key_ref, value_ref, low_ref, high_ref):
    width = key_ref.shape[1]
    run = (pos_ref[0] // run_rows).astype(F32)
    for half, out in enumerate((low_ref, high_ref)):
        rows = pl.ds(half * run_rows, run_rows)
        out[:run_rows, :width] = key_ref[rows, :]
        out[:run_rows, width:] = value_ref[rows, :]
        out[run_rows:, :] = jnp.full((TAG_ROWS, 2 * width), run, F32).astype(BF16)


def pack(positions, keys, values):
    run_rows = keys.shape[0] // 2
    shape = jax.ShapeDtypeStruct((run_rows + TAG_ROWS, 2 * keys.shape[1]), BF16)
    return pl.pallas_call(
        functools.partial(pack_body, run_rows),
        out_shape=(shape, shape),
        in_specs=[in_smem(), in_vmem(), in_vmem()],
        out_specs=(in_vmem(), in_vmem()),
        cost_estimate=cost(2e8, 4 * keys.size * 2),
        name="pack",
    )(positions, keys, values)


def attend_body(run_rows, runs, query_half, key_halves, count, *refs):
    pos_ref, query_ref = refs[:2]
    pieces = refs[2 : 2 + len(key_halves) * count]
    out_ref, kv_ref, hide_ref = refs[2 + len(key_halves) * count :]
    total = len(pieces) * run_rows
    kv_width = pieces[0].shape[1] // 2
    query_width = query_ref.shape[1]
    kv_heads = kv_width // HEAD
    group = query_width // kv_width
    step = (1.0 / math.sqrt(HEAD)) * math.log2(math.e)

    lane = lax.broadcasted_iota(jnp.int32, (1, total), 1)
    base = jnp.zeros((1, total), F32)
    first = jnp.zeros((1, total), jnp.int32)
    for number, piece in enumerate(pieces):
        kv_ref[pl.ds(number * run_rows, run_rows), :] = piece[:run_rows, :]
        tag = piece[run_rows : run_rows + TAG_ROWS, :HEAD].astype(F32)[:1, :]
        tag = jnp.concatenate([tag] * (total // HEAD), axis=1)
        if key_halves[number // count] == 1:
            tag = (runs - 1) - tag
        inside = lane >= number * run_rows
        base = jnp.where(inside, tag, base)
        first = jnp.where(inside, number * run_rows, first)
    key_pos = base * run_rows + (lane - first).astype(F32)
    run = pos_ref[0] // run_rows
    own_run = run if query_half == 0 else runs - 1 - run
    query_pos = (own_run * run_rows + lax.broadcasted_iota(jnp.int32, (run_rows, 1), 0)).astype(F32)
    hide_ref[...] = jnp.where(key_pos <= query_pos, 0.0, HIDE)

    pair = 2 if group % 2 == 0 else 1
    for kv_head in range(kv_heads):
        keys = kv_ref[:, kv_head * HEAD : (kv_head + 1) * HEAD]
        values = kv_ref[:, kv_width + kv_head * HEAD : kv_width + (kv_head + 1) * HEAD]
        for member in range(0, group, pair):
            heads = [kv_head * group + member + i for i in range(pair)]
            query = jnp.concatenate([query_ref[:, h * HEAD : (h + 1) * HEAD] for h in heads], axis=0)
            scores = lax.dot_general(query, keys, (((1,), (1,)), ((), ())), preferred_element_type=F32)
            weights, sums = [], []
            for i in range(pair):
                part = scores[i * run_rows : (i + 1) * run_rows] * step + hide_ref[...]
                part = jnp.exp2(part - jnp.max(part, axis=1, keepdims=True))
                sums.append(jnp.sum(part, axis=1, keepdims=True))
                weights.append(part.astype(BF16))
            mixed = jnp.dot(jnp.concatenate(weights, axis=0), values, preferred_element_type=F32)
            for i, h in enumerate(heads):
                mean = mixed[i * run_rows : (i + 1) * run_rows] / sums[i]
                out_ref[:, h * HEAD : (h + 1) * HEAD] = mean.astype(BF16)


def attend(positions, queries, query_half, piece_sets, key_halves, runs):
    run_rows = queries.shape[0] // 2
    count = len(piece_sets[0])
    pieces = [piece for pieces in piece_sets for piece in pieces]
    total = len(pieces) * run_rows
    width = queries.shape[1]
    return pl.pallas_call(
        functools.partial(attend_body, run_rows, runs, query_half, key_halves, count),
        out_shape=jax.ShapeDtypeStruct((run_rows, width), BF16),
        grid=(1,),
        in_specs=[in_smem(), pl.BlockSpec((run_rows, width), lambda i: (query_half, 0))]
        + [in_vmem()] * len(pieces),
        out_specs=pl.BlockSpec((run_rows, width), lambda i: (0, 0)),
        scratch_shapes=[
            VMEM((total, pieces[0].shape[1]), BF16),
            VMEM((run_rows, total), F32),
        ],
        cost_estimate=cost(4 * run_rows * total * width, total * pieces[0].shape[1] * 2),
        name=f"attend_{query_half}",
    )(positions, queries, *pieces)


def project_body(place_ref, att_ref, weight_ref, *rest):
    total = jnp.dot(att_ref[...], weight_ref[...], preferred_element_type=F32)
    if len(rest) > 1:
        arrived, residual = rest[0], rest[1]
        mine = jnp.where(place_ref[1] == 1, 1.0, 0.0).astype(F32)
        total = total.astype(BF16).astype(F32) + arrived[...].astype(F32)
        total = total + mine * residual[...].astype(F32)
    rest[-1][...] = total.astype(BF16)


def project(place, attended, weight, block_width, half=0, arrived=None, residual=None):
    rows, depth = attended.shape
    tile = math.gcd(block_width, 512)
    tiles = block_width // tile
    in_specs = [
        pl.BlockSpec((rows, depth), lambda i, place: (0, 0)),
        pl.BlockSpec((depth, tile), lambda i, place: (0, place[0] * tiles + i)),
    ]
    operands = [attended, weight]
    if arrived is not None:
        in_specs += [
            pl.BlockSpec((rows, tile), lambda i, place: (0, i)),
            pl.BlockSpec((rows, tile), lambda i, place: (half, i)),
        ]
        operands += [arrived, residual]
    return pl.pallas_call(
        project_body,
        out_shape=jax.ShapeDtypeStruct((rows, block_width), BF16),
        grid_spec=pltpu.PrefetchScalarGridSpec(
            num_scalar_prefetch=1,
            grid=(tiles,),
            in_specs=in_specs,
            out_specs=pl.BlockSpec((rows, tile), lambda i, place: (0, i)),
        ),
        cost_estimate=cost(2 * rows * depth * block_width, depth * block_width * 2),
        name="project_own" if arrived is not None else "project_other",
    )(place, *operands)


def finish_body(ny, cores, half, place_ref, gain_ref, *refs):
    blocks = ny * cores
    parts = refs[:blocks]
    refs = refs[blocks:]
    if half:
        scale_low_ref = refs[0]
        quant_ref, scale_ref, stream_ref = refs[-3:]
    else:
        quant_ref, scale_ref, stream_ref = refs[-3:]
    rows, width = parts[0].shape
    y, core = place_ref[0], place_ref[1]
    square = jnp.zeros((rows, 1), F32)
    peak = jnp.zeros((rows, 1), F32)
    stream = jnp.zeros((rows, width), F32)
    for yb in range(ny):
        stream = jnp.where(y == yb, parts[yb * cores][...].astype(F32), stream)
    stream_ref[...] = stream.astype(BF16)
    totals = []
    for b in range(blocks):
        value = parts[b][...].astype(F32)
        totals.append(jnp.sum(value * value, axis=1, keepdims=True))
    for yb in range(ny):
        for cb in range(cores):
            chosen = totals[yb * cores]
            for k in range(1, cores):
                chosen = jnp.where((core ^ k) == cb, totals[yb * cores + k], chosen)
            square = square + chosen
    root = lax.rsqrt(square / (blocks * width) + 1e-05)
    for yb in range(ny):
        for k in range(cores):
            value = parts[yb * cores + k][...].astype(F32) * root * gain_ref[(y ^ yb) * cores + k]
            peak = jnp.maximum(peak, jnp.max(jnp.abs(value), axis=1, keepdims=True))
    peak = peak + 1e-06
    for yb in range(ny):
        for k in range(cores):
            value = parts[yb * cores + k][...].astype(F32) * root * gain_ref[(y ^ yb) * cores + k]
            start = pl.multiple_of((yb * cores + (core ^ k)) * width, HEAD)
            quant_ref[:, pl.ds(start, width)] = (value / peak).astype(BF16)
    here = lax.broadcasted_iota(jnp.int32, (rows, rows), 0) == lax.broadcasted_iota(jnp.int32, (rows, rows), 1)
    line = jnp.sum(jnp.where(here, peak, 0.0), axis=0, keepdims=True)
    if half:
        scale_ref[0:1, :] = scale_low_ref[...]
        scale_ref[1:2, :] = line
    else:
        scale_ref[...] = line


def finish(ny, cores, half, place, gains, parts, earlier=None):
    rows, width = parts[0].shape
    blocks = ny * cores
    whole = lambda shape: pl.BlockSpec(shape, lambda i: (0,) * len(shape))
    out_shape = (
        jax.ShapeDtypeStruct((2 * rows, blocks * width), BF16),
        jax.ShapeDtypeStruct((1 + half, rows), F32),
        jax.ShapeDtypeStruct((2 * rows, width), BF16),
    )
    in_specs = [in_smem(), whole(gains.shape)] + [whole((rows, width))] * blocks
    operands = [place, gains, *parts]
    aliases = {}
    if half:
        in_specs += [whole((1, rows)), pl.BlockSpec(memory_space=pl.ANY), pl.BlockSpec(memory_space=pl.ANY)]
        aliases = {len(operands) + 1: 0, len(operands) + 2: 2}
        operands += [earlier[1], earlier[0], earlier[2]]
    return pl.pallas_call(
        functools.partial(finish_body, ny, cores, half),
        out_shape=out_shape,
        grid=(1,),
        in_specs=in_specs,
        out_specs=(
            pl.BlockSpec((rows, blocks * width), lambda i: (half, 0)),
            whole((1 + half, rows)),
            pl.BlockSpec((rows, width), lambda i: (half, 0)),
        ),
        input_output_aliases=aliases,
        cost_estimate=cost(2e9, 4 * rows * blocks * width),
        name=f"finish_{half}",
    )(*operands)


def swap(count, stride, distance):
    def partner(index):
        digit = (index // stride) % count[0]
        return index + ((digit ^ distance) - digit) * stride

    return [(index, partner(index)) for index in range(count[1])]


def on_device(sizes, queries, keys, values, positions, residual, norm_gain, out_weight):
    nz, nx, ny, cores = sizes
    n_seq, n_tp = nz * nx, ny * cores
    runs = 2 * n_seq
    block_width = residual.shape[1]
    tp = lax.axis_index("tp")
    y, core = tp // cores, tp % cores

    def move_z(array, k):
        return lax.ppermute(array, "seq", swap((nz, n_seq), nx, k))

    def move_x(array, k):
        return lax.ppermute(array, "seq", swap((nx, n_seq), 1, k))

    def move_y(array, k):
        return lax.ppermute(array, "tp", swap((ny, n_tp), cores, k))

    def move_core(array, k):
        return lax.ppermute(array, "tp", swap((cores, n_tp), 1, k))

    packed = pack(positions, keys, values)

    def gather(own):
        column = [own] + [move_z(own, k) for k in range(1, nz)]
        return column + [move_x(piece, k) for piece in column for k in range(1, nx)]

    low = gather(packed[0])
    high = gather(packed[1])

    near = [norm_gain] + [move_core(norm_gain, k) for k in range(1, cores)]
    near = jnp.stack(near)
    gains = jnp.concatenate([near] + [move_y(near, k) for k in range(1, ny)])
    place = jnp.stack([y, core])

    def place_of(yb, k):
        return jnp.stack([yb * cores + (core ^ k), (y == yb).astype(jnp.int32)])

    def tail(half, attended, earlier):
        sent = {}
        for yb in range(ny):
            for k in range(1, cores):
                sent[yb, k] = move_core(project(place_of(yb, k), attended, out_weight, block_width), k)
        parts = []
        for yb in range(ny):
            arrived = sent[yb, 1]
            own = project(place_of(yb, 0), attended, out_weight, block_width, half, arrived, residual)
            terms = [own] + [move_y(own, k) for k in range(1, ny)]
            terms = [term.astype(F32) for term in terms]
            while len(terms) > 1:
                terms = [terms[i] + terms[i + 1] for i in range(0, len(terms), 2)]
            whole = terms[0].astype(BF16)
            parts += [whole] + [move_core(whole, k) for k in range(1, cores)]
        return finish(ny, cores, half, place, gains, parts, earlier)

    early = attend(positions, queries, 0, [low], (0,), runs)
    first = tail(0, early, None)
    late = attend(positions, queries, 1, [low, high], (0, 1), runs)
    quantized, scale, stream = tail(1, late, first)
    return (quantized, scale.reshape(2 * scale.shape[1]), stream)


def sizes_of(mesh):
    along_seq, along_tp = list(mesh.devices[:, 0]), list(mesh.devices[0, :])
    nx = len({device.coords[0] for device in along_seq})
    ny = len({device.coords[1] for device in along_tp})
    return (len(along_seq) // nx, nx, ny, len(along_tp) // ny)


def solution(mesh):
    return jax.shard_map(
        functools.partial(on_device, sizes_of(mesh)),
        mesh=mesh,
        in_specs=(
            P("seq", "tp"),
            P("seq", "tp"),
            P("seq", "tp"),
            P("seq"),
            P("seq", "tp"),
            P(None, "tp"),
            P("tp", None),
        ),
        out_specs=(P("seq", None), P("seq"), P("seq", "tp")),
        check_vma=False,
    )
```

```python
import functools
import math

import jax
import jax.numpy as jnp
from jax import lax
from jax.experimental import pallas as pl
from jax.experimental.pallas import tpu as pltpu
from jax.sharding import PartitionSpec as P


HEAD = 128
TAG_ROWS = 8
HIDE = -1e30
VMEM = pltpu.VMEM
F32 = jnp.float32
BF16 = jnp.bfloat16


def in_vmem():
    return pl.BlockSpec(memory_space=VMEM)


def in_place():
    return pl.BlockSpec(memory_space=pl.ANY)


def near(array):
    return pltpu.with_memory_space_constraint(array, VMEM)


def far(array):
    return pltpu.with_memory_space_constraint(array, pltpu.HBM)


def after(array, *others):
    return lax.optimization_barrier((array, *others))[0]


def cost(flops, moved):
    return pl.CostEstimate(flops=int(flops), bytes_accessed=int(moved), transcendentals=0)


def grant(mib):
    return pltpu.CompilerParams(vmem_limit_bytes=mib << 20)


def run_copies(copies):
    for copy in copies:
        copy.start()
    for copy in copies:
        copy.wait()


def pack_body(run_rows, pos_ref, key_ref, value_ref, low_ref, high_ref, number_ref, sems):
    width = key_ref.shape[1]
    copies = [pltpu.make_async_copy(pos_ref, number_ref, sems.at[4])]
    for half, out in enumerate((low_ref, high_ref)):
        rows = pl.ds(half * run_rows, run_rows)
        for i, ref in enumerate((key_ref, value_ref)):
            target = out.at[pl.ds(0, run_rows), pl.ds(i * width, width)]
            copies.append(pltpu.make_async_copy(ref.at[rows, :], target, sems.at[2 * half + i]))
    for copy in copies:
        copy.start()
    copies[0].wait()
    run = (number_ref[0] // run_rows).astype(F32)
    for out in (low_ref, high_ref):
        out[run_rows:, :] = jnp.full((TAG_ROWS, 2 * width), run, F32).astype(BF16)
    for copy in copies[1:]:
        copy.wait()


def pack(positions, keys, values):
    run_rows = keys.shape[0] // 2
    shape = (run_rows + TAG_ROWS, 2 * keys.shape[1])
    return pl.pallas_call(
        functools.partial(pack_body, run_rows),
        out_shape=(VMEM(shape, BF16), VMEM(shape, BF16)),
        in_specs=[in_place()] * 3,
        out_specs=(in_vmem(), in_vmem()),
        scratch_shapes=[pltpu.SMEM(positions.shape, jnp.int32), pltpu.SemaphoreType.DMA((5,))],
        compiler_params=grant(4),
        cost_estimate=cost(2e8, 4 * keys.size * 2),
        name="pack",
    )(far(positions), far(keys), far(values))


def fetch_body(cores, blocks, width, weight_ref, *refs):
    extra = (len(refs) - 1 - len(blocks)) // 2
    outs, sems = refs[extra:-1], refs[-1]
    core = lax.axis_index("tp") % cores
    copies = []
    for i, (yb, k) in enumerate(blocks):
        start = pl.multiple_of((yb * cores + (core ^ k)) * width, HEAD)
        copies.append(pltpu.make_async_copy(weight_ref.at[:, pl.ds(start, width)], outs[i], sems.at[i]))
    for i in range(extra):
        at = len(blocks) + i
        copies.append(pltpu.make_async_copy(refs[i], outs[at], sems.at[at]))
    run_copies(copies)


def fetch(cores, blocks, width, weight, extra):
    shapes = [(weight.shape[0], width)] * len(blocks) + [array.shape for array in extra]
    return pl.pallas_call(
        functools.partial(fetch_body, cores, blocks, width),
        out_shape=tuple(VMEM(shape, BF16) for shape in shapes),
        in_specs=[in_place()] * (1 + len(extra)),
        out_specs=(in_vmem(),) * len(shapes),
        scratch_shapes=[pltpu.SemaphoreType.DMA((len(shapes),))],
        compiler_params=grant(4),
        cost_estimate=cost(2e9, 2 * weight.shape[0] * width * len(blocks)),
    )(far(weight), *[far(array) for array in extra])


def attend_body(run_rows, runs, query_half, key_halves, count, *refs):
    query_ref = refs[0]
    pieces = refs[1 : 1 + len(key_halves) * count]
    out_ref, kv_ref, hide_ref = refs[1 + len(key_halves) * count :]
    total = len(pieces) * run_rows
    kv_width = pieces[0].shape[1] // 2
    query_width = query_ref.shape[1]
    kv_heads = kv_width // HEAD
    group = query_width // kv_width
    step = (1.0 / math.sqrt(HEAD)) * math.log2(math.e)
    query_rows = pl.ds(query_half * run_rows, run_rows)

    lane = lax.broadcasted_iota(jnp.int32, (1, total), 1)
    base = jnp.zeros((1, total), F32)
    first = jnp.zeros((1, total), jnp.int32)
    own = None
    for number, piece in enumerate(pieces):
        kv_ref[pl.ds(number * run_rows, run_rows), :] = piece[:run_rows, :]
        tag = piece[run_rows : run_rows + TAG_ROWS, :HEAD].astype(F32)[:1, :]
        if number == 0:
            own = tag[:, :1]
        tag = jnp.concatenate([tag] * (total // HEAD), axis=1)
        if key_halves[number // count] == 1:
            tag = (runs - 1) - tag
        inside = lane >= number * run_rows
        base = jnp.where(inside, tag, base)
        first = jnp.where(inside, number * run_rows, first)
    key_pos = base * run_rows + (lane - first).astype(F32)
    own = own if query_half == 0 else runs - 1 - own
    query_pos = own * run_rows + lax.broadcasted_iota(jnp.int32, (run_rows, 1), 0).astype(F32)
    hide_ref[...] = jnp.where(key_pos <= query_pos, 0.0, HIDE)

    pair = 2 if group % 2 == 0 else 1
    for kv_head in range(kv_heads):
        keys = kv_ref[:, kv_head * HEAD : (kv_head + 1) * HEAD]
        values = kv_ref[:, kv_width + kv_head * HEAD : kv_width + (kv_head + 1) * HEAD]
        for member in range(0, group, pair):
            heads = [kv_head * group + member + i for i in range(pair)]
            query = jnp.concatenate([query_ref[query_rows, h * HEAD : (h + 1) * HEAD] for h in heads], axis=0)
            scores = lax.dot_general(query, keys, (((1,), (1,)), ((), ())), preferred_element_type=F32)
            weights, sums = [], []
            for i in range(pair):
                part = scores[i * run_rows : (i + 1) * run_rows] * step + hide_ref[...]
                part = jnp.exp2(part - jnp.max(part, axis=1, keepdims=True))
                sums.append(jnp.sum(part, axis=1, keepdims=True))
                weights.append(part.astype(BF16))
            mixed = jnp.dot(jnp.concatenate(weights, axis=0), values, preferred_element_type=F32)
            for i, h in enumerate(heads):
                mean = mixed[i * run_rows : (i + 1) * run_rows] / sums[i]
                out_ref[:, h * HEAD : (h + 1) * HEAD] = mean.astype(BF16)


def attend(queries, query_half, piece_sets, key_halves, runs):
    run_rows = queries.shape[0] // 2
    count = len(piece_sets[0])
    pieces = [near(piece) for pieces in piece_sets for piece in pieces]
    total = len(pieces) * run_rows
    width = queries.shape[1]
    return pl.pallas_call(
        functools.partial(attend_body, run_rows, runs, query_half, key_halves, count),
        out_shape=VMEM((run_rows, width), BF16),
        in_specs=[in_vmem()] * (1 + len(pieces)),
        out_specs=in_vmem(),
        scratch_shapes=[
            VMEM((total, pieces[0].shape[1]), BF16),
            VMEM((run_rows, total), F32),
        ],
        compiler_params=grant(12),
        cost_estimate=cost(4 * run_rows * total * width, total * pieces[0].shape[1] * 2),
    )(near(queries), *pieces)


def project_body(cores, blocks, half, own, att_ref, *rest):
    weights, rest = rest[: len(blocks)], rest[len(blocks) :]
    outs = rest[2:] if own else rest
    width = weights[0].shape[1]
    tp = lax.axis_index("tp")
    for i, yb in enumerate(blocks):
        total = jnp.dot(att_ref[...], weights[i][...], preferred_element_type=F32)
        columns = slice(i * width, (i + 1) * width)
        if own:
            arrived, residual = rest[0], rest[1]
            mine = jnp.where(tp // cores == yb, 1.0, 0.0).astype(F32)
            total = total.astype(BF16).astype(F32) + arrived[:, columns].astype(F32)
            rows = pl.ds(half * arrived.shape[0], arrived.shape[0])
            total = total + mine * residual[rows, :].astype(F32)
        total = total.astype(BF16)
        rows = outs[0].shape[0]
        for j, out in enumerate(outs):
            out[:, columns] = total[j * rows : (j + 1) * rows]


def project(cores, blocks, half, attended, weights, cuts=1, arrived=None, residual=None):
    rows, depth = attended.shape
    width = weights[0].shape[1] * len(blocks)
    own = arrived is not None
    operands = [attended, *weights] + ([arrived, residual] if own else [])
    result = pl.pallas_call(
        functools.partial(project_body, cores, blocks, half, own),
        out_shape=(VMEM((rows // cuts, width), BF16),) * cuts,
        in_specs=[in_vmem()] * len(operands),
        out_specs=(in_vmem(),) * cuts,
        compiler_params=grant(8),
        cost_estimate=cost(2 * rows * depth * width, depth * width * 2),
        name="project_own" if own else "project_other",
    )(*[near(operand) for operand in operands])
    return result if cuts > 1 else result[0]


def finish_body(ny, cores, row, places, count, gain_ref, *refs):
    parts = refs[:count]
    line_ref = refs[count]
    quant_ref, line_out, stream_ref, quant_vmem, stream_vmem, sems = refs[-6:]
    rows = parts[0].shape[0]
    blocks = ny * cores
    width = gain_ref.shape[2]
    tp = lax.axis_index("tp")
    y, core = tp // cores, tp % cores

    def part(yb, k):
        number, column = places[yb, k]
        return parts[number][:, column * width : (column + 1) * width].astype(F32)

    stream = part(0, 0)
    for yb in range(1, ny):
        stream = jnp.where(y == yb, part(yb, 0), stream)
    stream_vmem[...] = stream.astype(BF16)
    copies = [pltpu.make_async_copy(stream_vmem, stream_ref.at[pl.ds(row, rows), :], sems.at[blocks])]
    copies[0].start()
    totals = {}
    for yb in range(ny):
        for k in range(cores):
            value = part(yb, k)
            totals[yb, k] = jnp.sum(value * value, axis=1, keepdims=True)
    square = jnp.zeros((rows, 1), F32)
    for yb in range(ny):
        for cb in range(cores):
            chosen = totals[yb, 0]
            for k in range(1, cores):
                chosen = jnp.where((core ^ k) == cb, totals[yb, k], chosen)
            square = square + chosen
    root = lax.rsqrt(square / (blocks * width) + 1e-05)
    peak = jnp.zeros((rows, 1), F32)
    for yb in range(ny):
        for k in range(cores):
            value = part(yb, k) * gain_ref[(y ^ yb) * cores + k]
            peak = jnp.maximum(peak, jnp.max(jnp.abs(value), axis=1, keepdims=True))
    peak = peak * root + 1e-06
    factor = root / peak
    for yb in range(ny):
        for k in range(cores):
            value = part(yb, k) * gain_ref[(y ^ yb) * cores + k] * factor
            slot = yb * cores + k
            start = pl.multiple_of((yb * cores + (core ^ k)) * width, HEAD)
            quant_vmem[slot] = value.astype(BF16)
            target = quant_ref.at[pl.ds(row, rows), pl.ds(start, width)]
            copies.append(pltpu.make_async_copy(quant_vmem.at[slot], target, sems.at[slot]))
            copies[-1].start()
    lanes = line_out.shape[-1]
    lane = lax.broadcasted_iota(jnp.int32, (rows, lanes), 1)
    here = lax.broadcasted_iota(jnp.int32, (rows, lanes), 0) + row == lane
    line = jnp.sum(jnp.where(here, peak, 0.0), axis=0, keepdims=True)
    if row:
        line = line + line_ref[...]
    line_out[...] = line.reshape(line_out.shape)
    for copy in copies:
        copy.wait()


def finish(ny, cores, row, all_rows, gains, parts, places, earlier, last):
    rows = parts[0].shape[0]
    width = gains.shape[2]
    blocks = ny * cores
    operands = [near(gains), *[near(part) for part in parts]]
    line = (all_rows,) if last else (1, all_rows)
    out_shape = (
        jax.ShapeDtypeStruct((all_rows, blocks * width), BF16),
        jax.ShapeDtypeStruct(line, F32) if last else VMEM(line, F32),
        jax.ShapeDtypeStruct((all_rows, width), BF16),
    )
    aliases = {}
    if earlier is not None:
        aliases = {len(operands) + 1: 0, len(operands) + 2: 2}
        operands += [near(earlier[1]), earlier[0], earlier[2]]
    else:
        operands += [near(jnp.zeros((1, all_rows), F32))]
    n = 2 + len(parts)
    return pl.pallas_call(
        functools.partial(finish_body, ny, cores, row, places, len(parts)),
        out_shape=out_shape,
        in_specs=[in_vmem()] * n + [in_place()] * (len(operands) - n),
        out_specs=(in_place(), in_vmem(), in_place()),
        scratch_shapes=[
            VMEM((blocks, rows, width), BF16),
            VMEM((rows, width), BF16),
            pltpu.SemaphoreType.DMA((blocks + 1,)),
        ],
        input_output_aliases=aliases,
        compiler_params=grant(8),
        cost_estimate=cost(2e9, 4 * rows * blocks * width),
    )(*operands)


def swap(size, count, stride, distance):
    def partner(index):
        digit = (index // stride) % size
        return index + ((digit ^ distance) - digit) * stride

    return [(index, partner(index)) for index in range(count)]


def tree_sum(terms):
    terms = [term.astype(F32) for term in terms]
    while len(terms) > 1:
        terms = [terms[i] + terms[i + 1] for i in range(0, len(terms), 2)]
    return terms[0].astype(BF16)


def on_device(sizes, queries, keys, values, positions, residual, norm_gain, out_weight):
    nz, nx, ny, cores = sizes
    n_seq, n_tp = nz * nx, ny * cores
    runs = 2 * n_seq
    all_rows, block_width = residual.shape
    run_rows = all_rows // 2

    def move_z(array, k):
        return lax.ppermute(array, "seq", swap(nz, n_seq, nx, k))

    def move_x(array, k):
        return lax.ppermute(array, "seq", swap(nx, n_seq, 1, k))

    def move_y(array, k):
        return lax.ppermute(array, "tp", swap(ny, n_tp, cores, k))

    def move_core(array, k):
        return lax.ppermute(array, "tp", swap(cores, n_tp, 1, k))

    low, high = pack(positions, keys, values)
    low_pieces = [low] + [move_x(low, j) for j in range(1, nx)]
    weights = {}

    def held_until_a(piece):
        if "a" not in state:
            source = after(out_weight, near_block)
            *blocks, state["query"] = fetch(cores, [(0, 1)], block_width, source, [queries])
            weights[0, 1] = blocks[0]
            state["a"] = blocks[0]
        return after(piece, state["a"])

    state = {}
    near_block = None
    step, column = nz // 2, [low]
    firsts = {k: move_z(low, k) for k in dict.fromkeys((step, 1)) if k}
    near_block = firsts[1]
    while step:
        for held in list(column):
            if held is low and step in firsts:
                column.append(firsts[step])
            else:
                column.append(move_z(held_until_a(held), step))
        step //= 2
    for piece in column[1:]:
        gate = piece if piece is near_block else after(piece, state.get("a", near_block))
        low_pieces += [piece] + [move_x(gate, j) for j in range(1, nx)]
    if "query" not in state:
        held_until_a(low)
    query_near = state["query"]

    source = after(out_weight, state["a"])
    rest = [(yb, 1) for yb in range(1, ny)]
    *blocks, residual_near = fetch(cores, rest, block_width, source, [residual])
    weights.update(zip(rest, blocks))
    source = after(out_weight, residual_near, column[-1])
    rest = [(yb, 0) for yb in range(ny)]
    weights.update(zip(rest, fetch(cores, rest, block_width, source, [])))

    early = attend(query_near, 0, [low_pieces], (0,), runs)
    sent, parts, marks = [], [], []
    for yb in range(ny):
        other = project(cores, [yb], 0, early, [weights[yb, 1]])
        sent.append(move_core(other, 1))
    for yb in range(ny):
        own = project(cores, [yb], 0, early, [weights[yb, 0]], 1, sent[yb], residual_near)
        marks.append(own)
        total = tree_sum([own] + [move_y(own, k) for k in range(1, ny)])
        parts += [total, move_core(total, 1)]
    places = {(yb, k): (yb * cores + k, 0) for yb in range(ny) for k in range(cores)}
    pair = [norm_gain] + [move_core(after(norm_gain, marks[0]), k) for k in range(1, cores)]
    pair = jnp.stack(pair)
    gains = jnp.concatenate([pair] + [move_y(pair, k) for k in range(1, ny)])
    result = finish(ny, cores, 0, all_rows, gains, parts, places, None, False)

    step, column = nz // 2, [high]
    ready = after(high, state["a"])
    firsts = {k: move_z(ready, k) for k in dict.fromkeys((step, 1)) if k}
    while step:
        for held in list(column):
            if held is high and step in firsts:
                column.append(firsts[step])
            else:
                column.append(move_z(after(held, marks[0]), step))
        step //= 2
    high_pieces = []
    for piece in column:
        high_pieces += [piece] + [move_x(after(piece, marks[0]), j) for j in range(1, nx)]

    late = attend(query_near, 1, [low_pieces, high_pieces], (0, 1), runs)
    every = list(range(ny))
    other = project(cores, every, 1, late, [weights[yb, 1] for yb in every])
    arrived = move_core(other, 1)
    cuts = project(cores, every, 1, late, [weights[yb, 0] for yb in every], 2, arrived, residual_near)
    places = {(yb, k): (k, yb) for yb in range(ny) for k in range(cores)}
    for i, own in enumerate(cuts):
        total = tree_sum([own] + [move_y(own, k) for k in range(1, ny)])
        parts = [total, move_core(total, 1)]
        row = run_rows + i * own.shape[0]
        result = finish(ny, cores, row, all_rows, gains, parts, places, result, i == 1)
    quantized, scale, stream = result
    return (quantized, scale, stream)


def sizes_of(mesh):
    along_seq, along_tp = list(mesh.devices[:, 0]), list(mesh.devices[0, :])
    nx = len({device.coords[0] for device in along_seq})
    ny = len({device.coords[1] for device in along_tp})
    return (len(along_seq) // nx, nx, ny, len(along_tp) // ny)


def solution(mesh):
    return jax.shard_map(
        functools.partial(on_device, sizes_of(mesh)),
        mesh=mesh,
        in_specs=(
            P("seq", "tp"),
            P("seq", "tp"),
            P("seq", "tp"),
            P("seq"),
            P("seq", "tp"),
            P(None, "tp"),
            P("tp", None),
        ),
        out_specs=(P("seq", None), P("seq"), P("seq", "tp")),
        check_vma=False,
    )
```

```python
import functools
import math

import jax
import jax.numpy as jnp
from jax import lax
from jax.experimental import pallas as pl
from jax.experimental.pallas import tpu as pltpu
from jax.sharding import PartitionSpec as P


HEAD = 128
TAG_ROWS = 8
HIDE = -1e30
VMEM = pltpu.VMEM
F32 = jnp.float32
BF16 = jnp.bfloat16


def in_vmem():
    return pl.BlockSpec(memory_space=VMEM)


def in_place():
    return pl.BlockSpec(memory_space=pl.ANY)


def near(array):
    return pltpu.with_memory_space_constraint(array, VMEM)


def far(array):
    return pltpu.with_memory_space_constraint(array, pltpu.HBM)


def after(array, *others):
    return lax.optimization_barrier((array, *others))[0]


def cost(flops, moved):
    return pl.CostEstimate(flops=int(flops), bytes_accessed=int(moved), transcendentals=0)


def grant(mib):
    return pltpu.CompilerParams(vmem_limit_bytes=mib << 20)


def pack_body(run_rows, pos_ref, key_ref, value_ref, low_ref, high_ref, number_ref, sems):
    width = key_ref.shape[1]
    copies = [pltpu.make_async_copy(pos_ref, number_ref, sems.at[4])]
    for half, out in enumerate((low_ref, high_ref)):
        rows = pl.ds(half * run_rows, run_rows)
        for i, ref in enumerate((key_ref, value_ref)):
            target = out.at[pl.ds(0, run_rows), pl.ds(i * width, width)]
            copies.append(pltpu.make_async_copy(ref.at[rows, :], target, sems.at[2 * half + i]))
    for copy in copies:
        copy.start()
    copies[0].wait()
    run = (number_ref[0] // run_rows).astype(F32)
    for out in (low_ref, high_ref):
        out[run_rows:, :] = jnp.full((TAG_ROWS, 2 * width), run, F32).astype(BF16)
    for copy in copies[1:]:
        copy.wait()


def pack(positions, keys, values):
    run_rows = keys.shape[0] // 2
    shape = (run_rows + TAG_ROWS, 2 * keys.shape[1])
    return pl.pallas_call(
        functools.partial(pack_body, run_rows),
        out_shape=(VMEM(shape, BF16), VMEM(shape, BF16)),
        in_specs=[in_place()] * 3,
        out_specs=(in_vmem(), in_vmem()),
        scratch_shapes=[pltpu.SMEM(positions.shape, jnp.int32), pltpu.SemaphoreType.DMA((5,))],
        compiler_params=grant(4),
        cost_estimate=cost(4e10, 4 * keys.size * 2),
        name="pack",
    )(far(positions), far(keys), far(values))


def join_body(*refs):
    rows = refs[0].shape[0]
    for i, ref in enumerate(refs[:-1]):
        refs[-1][i * rows : (i + 1) * rows, :] = ref[...]


def join(pieces):
    rows, width = pieces[0].shape
    return pl.pallas_call(
        join_body,
        out_shape=VMEM((len(pieces) * rows, width), BF16),
        in_specs=[in_vmem()] * len(pieces),
        out_specs=in_vmem(),
        compiler_params=grant(4),
        cost_estimate=cost(2e8, 4 * len(pieces) * rows * width),
        name="join",
    )(*[near(piece) for piece in pieces])


def attend_body(run_rows, runs, query_half, key_halves, *refs):
    query_ref = refs[0]
    pieces = refs[1 : 1 + len(key_halves)]
    out_ref, kv_ref, hide_ref = refs[1 + len(key_halves) :]
    block_rows = run_rows + TAG_ROWS
    held = [
        (piece, row, half)
        for piece, half in zip(pieces, key_halves)
        for row in range(0, piece.shape[0], block_rows)
    ]
    total = len(held) * run_rows
    kv_width = pieces[0].shape[1] // 2
    query_width = query_ref.shape[1]
    kv_heads = kv_width // HEAD
    group = query_width // kv_width
    step = (1.0 / math.sqrt(HEAD)) * math.log2(math.e)
    query_rows = pl.ds(query_half * run_rows, run_rows)

    lane = lax.broadcasted_iota(jnp.int32, (1, total), 1)
    base = jnp.zeros((1, total), F32)
    first = jnp.zeros((1, total), jnp.int32)
    own = None
    for number, (piece, row, half) in enumerate(held):
        kv_ref[pl.ds(number * run_rows, run_rows), :] = piece[row : row + run_rows, :]
        tag = piece[row + run_rows : row + block_rows, :HEAD].astype(F32)[:1, :]
        if number == 0:
            own = tag[:, :1]
        tag = jnp.concatenate([tag] * (total // HEAD), axis=1)
        if half == 1:
            tag = (runs - 1) - tag
        inside = lane >= number * run_rows
        base = jnp.where(inside, tag, base)
        first = jnp.where(inside, number * run_rows, first)
    key_pos = base * run_rows + (lane - first).astype(F32)
    own = own if query_half == 0 else runs - 1 - own
    query_pos = own * run_rows + lax.broadcasted_iota(jnp.int32, (run_rows, 1), 0).astype(F32)
    hide_ref[...] = jnp.where(key_pos <= query_pos, 0.0, HIDE)

    pair = 2 if group % 2 == 0 else 1
    for kv_head in range(kv_heads):
        keys = kv_ref[:, kv_head * HEAD : (kv_head + 1) * HEAD]
        values = kv_ref[:, kv_width + kv_head * HEAD : kv_width + (kv_head + 1) * HEAD]
        for member in range(0, group, pair):
            heads = [kv_head * group + member + i for i in range(pair)]
            query = jnp.concatenate([query_ref[query_rows, h * HEAD : (h + 1) * HEAD] for h in heads], axis=0)
            scores = lax.dot_general(query, keys, (((1,), (1,)), ((), ())), preferred_element_type=F32)
            weights, sums = [], []
            for i in range(pair):
                part = scores[i * run_rows : (i + 1) * run_rows] * step + hide_ref[...]
                part = jnp.exp2(part - jnp.max(part, axis=1, keepdims=True))
                sums.append(jnp.sum(part, axis=1, keepdims=True))
                weights.append(part.astype(BF16))
            mixed = jnp.dot(jnp.concatenate(weights, axis=0), values, preferred_element_type=F32)
            for i, h in enumerate(heads):
                mean = mixed[i * run_rows : (i + 1) * run_rows] / sums[i]
                out_ref[:, h * HEAD : (h + 1) * HEAD] = mean.astype(BF16)


def attend(queries, query_half, piece_sets, runs):
    run_rows = queries.shape[0] // 2
    key_halves = [half for half, pieces in enumerate(piece_sets) for piece in pieces]
    pieces = [near(piece) for pieces in piece_sets for piece in pieces]
    total = sum(piece.shape[0] for piece in pieces) // (run_rows + TAG_ROWS) * run_rows
    width = queries.shape[1]
    return pl.pallas_call(
        functools.partial(attend_body, run_rows, runs, query_half, key_halves),
        out_shape=VMEM((run_rows, width), BF16),
        in_specs=[in_vmem()] * (1 + len(pieces)),
        out_specs=in_vmem(),
        scratch_shapes=[
            VMEM((total, pieces[0].shape[1]), BF16),
            VMEM((run_rows, total), F32),
        ],
        compiler_params=grant(12),
        cost_estimate=cost(4 * run_rows * total * width, total * pieces[0].shape[1] * 2),
    )(near(queries), *pieces)


def project_body(cores, blocks, half, own, att_ref, weight_ref, *rest):
    outs = rest[2:] if own else rest
    width = outs[0].shape[1] // len(blocks)
    tp = lax.axis_index("tp")
    for i, yb in enumerate(blocks):
        block = yb * cores + ((tp % cores) ^ (0 if own else 1))
        start = pl.multiple_of(block * width, HEAD)
        total = jnp.dot(att_ref[...], weight_ref[:, pl.ds(start, width)], preferred_element_type=F32)
        columns = slice(i * width, (i + 1) * width)
        if own:
            arrived, residual = rest[0], rest[1]
            mine = jnp.where(tp // cores == yb, 1.0, 0.0).astype(F32)
            total = total.astype(BF16).astype(F32) + arrived[:, columns].astype(F32)
            rows = pl.ds(half * arrived.shape[0], arrived.shape[0])
            total = total + mine * residual[rows, :].astype(F32)
        total = total.astype(BF16)
        rows = outs[0].shape[0]
        for j, out in enumerate(outs):
            out[:, columns] = total[j * rows : (j + 1) * rows]


def project(cores, blocks, half, attended, weight, block_width, cuts=1, arrived=None, residual=None):
    rows, depth = attended.shape
    width = block_width * len(blocks)
    own = arrived is not None
    operands = [attended, weight] + ([arrived, residual] if own else [])
    result = pl.pallas_call(
        functools.partial(project_body, cores, blocks, half, own),
        out_shape=(VMEM((rows // cuts, width), BF16),) * cuts,
        in_specs=[in_vmem()] * len(operands),
        out_specs=(in_vmem(),) * cuts,
        compiler_params=grant(8),
        cost_estimate=cost(2 * rows * depth * width, depth * width * 2),
        name="project_own" if own else "project_other",
    )(*[near(operand) for operand in operands])
    return result if cuts > 1 else result[0]


def finish_body(ny, cores, row, places, count, gain_ref, *refs):
    parts = refs[:count]
    line_ref = refs[count]
    quant_ref, line_out, stream_ref, quant_vmem, stream_vmem, sems = refs[-6:]
    rows = parts[0].shape[0]
    blocks = ny * cores
    width = gain_ref.shape[2]
    tp = lax.axis_index("tp")
    y, core = tp // cores, tp % cores

    def part(yb, k):
        number, column = places[yb, k]
        return parts[number][:, column * width : (column + 1) * width].astype(F32)

    stream = part(0, 0)
    for yb in range(1, ny):
        stream = jnp.where(y == yb, part(yb, 0), stream)
    stream_vmem[...] = stream.astype(BF16)
    copies = [pltpu.make_async_copy(stream_vmem, stream_ref.at[pl.ds(row, rows), :], sems.at[blocks])]
    copies[0].start()
    totals = {}
    for yb in range(ny):
        for k in range(cores):
            value = part(yb, k)
            totals[yb, k] = jnp.sum(value * value, axis=1, keepdims=True)
    square = jnp.zeros((rows, 1), F32)
    for yb in range(ny):
        for cb in range(cores):
            chosen = totals[yb, 0]
            for k in range(1, cores):
                chosen = jnp.where((core ^ k) == cb, totals[yb, k], chosen)
            square = square + chosen
    root = lax.rsqrt(square / (blocks * width) + 1e-05)
    peak = jnp.zeros((rows, 1), F32)
    for yb in range(ny):
        for k in range(cores):
            value = part(yb, k) * gain_ref[(y ^ yb) * cores + k]
            peak = jnp.maximum(peak, jnp.max(jnp.abs(value), axis=1, keepdims=True))
    peak = peak * root + 1e-06
    factor = root / peak
    for yb in range(ny):
        for k in range(cores):
            value = part(yb, k) * gain_ref[(y ^ yb) * cores + k] * factor
            slot = yb * cores + k
            start = pl.multiple_of((yb * cores + (core ^ k)) * width, HEAD)
            quant_vmem[slot] = value.astype(BF16)
            target = quant_ref.at[pl.ds(row, rows), pl.ds(start, width)]
            copies.append(pltpu.make_async_copy(quant_vmem.at[slot], target, sems.at[slot]))
            copies[-1].start()
    lanes = line_out.shape[-1]
    lane = lax.broadcasted_iota(jnp.int32, (rows, lanes), 1)
    here = lax.broadcasted_iota(jnp.int32, (rows, lanes), 0) + row == lane
    line = jnp.sum(jnp.where(here, peak, 0.0), axis=0, keepdims=True)
    if row:
        line = line + line_ref[...]
    line_out[...] = line.reshape(line_out.shape)
    for copy in copies:
        copy.wait()


def finish(ny, cores, row, all_rows, gains, parts, places, earlier, last):
    rows = parts[0].shape[0]
    width = gains.shape[2]
    blocks = ny * cores
    operands = [near(gains), *[near(part) for part in parts]]
    line = (all_rows,) if last else (1, all_rows)
    out_shape = (
        jax.ShapeDtypeStruct((all_rows, blocks * width), BF16),
        jax.ShapeDtypeStruct(line, F32) if last else VMEM(line, F32),
        jax.ShapeDtypeStruct((all_rows, width), BF16),
    )
    aliases = {}
    if earlier is not None:
        aliases = {len(operands) + 1: 0, len(operands) + 2: 2}
        operands += [near(earlier[1]), earlier[0], earlier[2]]
    else:
        operands += [near(jnp.zeros((1, all_rows), F32))]
    n = 2 + len(parts)
    return pl.pallas_call(
        functools.partial(finish_body, ny, cores, row, places, len(parts)),
        out_shape=out_shape,
        in_specs=[in_vmem()] * n + [in_place()] * (len(operands) - n),
        out_specs=(in_place(), in_vmem(), in_place()),
        scratch_shapes=[
            VMEM((blocks, rows, width), BF16),
            VMEM((rows, width), BF16),
            pltpu.SemaphoreType.DMA((blocks + 1,)),
        ],
        input_output_aliases=aliases,
        compiler_params=grant(8),
        cost_estimate=cost(2e9, 4 * rows * blocks * width),
    )(*operands)


def swap(size, count, stride, distance):
    def partner(index):
        digit = (index // stride) % size
        return index + ((digit ^ distance) - digit) * stride

    return [(index, partner(index)) for index in range(count)]


def tree_sum(terms):
    terms = [term.astype(F32) for term in terms]
    while len(terms) > 1:
        terms = [terms[i] + terms[i + 1] for i in range(0, len(terms), 2)]
    return terms[0].astype(BF16)


def on_device(sizes, queries, keys, values, positions, residual, norm_gain, out_weight):
    nz, nx, ny, cores = sizes
    n_seq, n_tp = nz * nx, ny * cores
    runs = 2 * n_seq
    all_rows, block_width = residual.shape
    run_rows = all_rows // 2

    def move_z(array, k):
        return lax.ppermute(array, "seq", swap(nz, n_seq, nx, k))

    def move_x(array, k):
        return lax.ppermute(array, "seq", swap(nx, n_seq, 1, k))

    def move_y(array, k):
        return lax.ppermute(array, "tp", swap(ny, n_tp, cores, k))

    def move_core(array, k):
        return lax.ppermute(array, "tp", swap(cores, n_tp, 1, k))

    low, high = pack(positions, keys, values)
    low_pieces = [low] + [move_x(low, j) for j in range(1, nx)]

    step, column = nz // 2, [low]
    firsts = {k: move_z(low, k) for k in dict.fromkeys((step, 1)) if k}
    while step:
        for held in list(column):
            if held is low and step in firsts:
                column.append(firsts[step])
            else:
                column.append(move_z(held, step))
        step //= 2
    for piece in column[1:]:
        low_pieces += [piece] + [move_x(piece, j) for j in range(1, nx)]

    high_line = [high] + [move_x(high, j) for j in range(1, nx)]
    high_line = join([after(high_line[0], firsts[1]), *high_line[1:]])
    step, high_pieces = nz // 2, [high_line]
    firsts = {k: move_z(high_line, k) for k in dict.fromkeys((step, 1)) if k}
    while step:
        for held in list(high_pieces):
            if held is high_line and step in firsts:
                high_pieces.append(firsts[step])
            else:
                high_pieces.append(move_z(held, step))
        step //= 2

    early = attend(queries, 0, [low_pieces], runs)
    sent, parts, marks = [], [], []
    for yb in range(ny):
        other = project(cores, [yb], 0, early, out_weight, block_width)
        sent.append(move_core(other, 1))
    for yb in range(ny):
        own = project(cores, [yb], 0, early, out_weight, block_width, 1, sent[yb], residual)
        marks.append(own)
        total = tree_sum([own] + [move_y(own, k) for k in range(1, ny)])
        parts += [total, move_core(total, 1)]
    places = {(yb, k): (yb * cores + k, 0) for yb in range(ny) for k in range(cores)}
    pair = [norm_gain] + [move_core(after(norm_gain, marks[0]), k) for k in range(1, cores)]
    pair = jnp.stack(pair)
    gains = jnp.concatenate([pair] + [move_y(pair, k) for k in range(1, ny)])
    result = finish(ny, cores, 0, all_rows, gains, parts, places, None, False)

    late = attend(queries, 1, [low_pieces, high_pieces], runs)
    every = list(range(ny))
    other = project(cores, every, 1, late, out_weight, block_width)
    arrived = move_core(other, 1)
    cuts = project(cores, every, 1, late, out_weight, block_width, 2, arrived, residual)
    places = {(yb, k): (k, yb) for yb in range(ny) for k in range(cores)}
    for i, own in enumerate(cuts):
        total = tree_sum([own] + [move_y(own, k) for k in range(1, ny)])
        parts = [total, move_core(total, 1)]
        row = run_rows + i * own.shape[0]
        result = finish(ny, cores, row, all_rows, gains, parts, places, result, i == 1)
    quantized, scale, stream = result
    return (quantized, scale, stream)


def sizes_of(mesh):
    along_seq, along_tp = list(mesh.devices[:, 0]), list(mesh.devices[0, :])
    nx = len({device.coords[0] for device in along_seq})
    ny = len({device.coords[1] for device in along_tp})
    return (len(along_seq) // nx, nx, ny, len(along_tp) // ny)


def solution(mesh):
    return jax.shard_map(
        functools.partial(on_device, sizes_of(mesh)),
        mesh=mesh,
        in_specs=(
            P("seq", "tp"),
            P("seq", "tp"),
            P("seq", "tp"),
            P("seq"),
            P("seq", "tp"),
            P(None, "tp"),
            P("tp", None),
        ),
        out_specs=(P("seq", None), P("seq"), P("seq", "tp")),
        check_vma=False,
    )
```

```python
import functools
import math

import jax
import jax.numpy as jnp
from jax import lax
from jax.experimental import pallas as pl
from jax.experimental.pallas import tpu as pltpu
from jax.sharding import PartitionSpec as P


HEAD = 128
TAG_ROWS = 8
HIDE = -1e30
CUTS = (1, 1)
VMEM = pltpu.VMEM
F32 = jnp.float32
BF16 = jnp.bfloat16


def in_vmem():
    return pl.BlockSpec(memory_space=VMEM)


def in_place():
    return pl.BlockSpec(memory_space=pl.ANY)


def near(array):
    return pltpu.with_memory_space_constraint(array, VMEM)


def far(array):
    return pltpu.with_memory_space_constraint(array, pltpu.HBM)


def after(array, *others):
    return lax.optimization_barrier((array, *others))[0]


def cost(flops, moved):
    return pl.CostEstimate(flops=int(flops), bytes_accessed=int(moved), transcendentals=0)


def grant(mib):
    return pltpu.CompilerParams(vmem_limit_bytes=mib << 20)


def pack_body(run_rows, pos_ref, key_ref, value_ref, low_ref, high_ref, number_ref, sems):
    width = key_ref.shape[1]
    copies = [pltpu.make_async_copy(pos_ref, number_ref, sems.at[4])]
    for half, out in enumerate((low_ref, high_ref)):
        rows = pl.ds(half * run_rows, run_rows)
        for i, ref in enumerate((key_ref, value_ref)):
            target = out.at[pl.ds(0, run_rows), pl.ds(i * width, width)]
            copies.append(pltpu.make_async_copy(ref.at[rows, :], target, sems.at[2 * half + i]))
    for copy in copies:
        copy.start()
    copies[0].wait()
    run = (number_ref[0] // run_rows).astype(F32)
    for out in (low_ref, high_ref):
        out[run_rows:, :] = jnp.full((TAG_ROWS, 2 * width), run, F32).astype(BF16)
    for copy in copies[1:]:
        copy.wait()


def pack(positions, keys, values):
    run_rows = keys.shape[0] // 2
    shape = (run_rows + TAG_ROWS, 2 * keys.shape[1])
    return pl.pallas_call(
        functools.partial(pack_body, run_rows),
        out_shape=(VMEM(shape, BF16), VMEM(shape, BF16)),
        in_specs=[in_place()] * 3,
        out_specs=(in_vmem(), in_vmem()),
        scratch_shapes=[pltpu.SMEM(positions.shape, jnp.int32), pltpu.SemaphoreType.DMA((5,))],
        compiler_params=grant(4),
        cost_estimate=cost(4e10, 4 * keys.size * 2),
        name="pack",
    )(far(positions), far(keys), far(values))


def join_body(*refs):
    rows = refs[0].shape[0]
    for i, ref in enumerate(refs[:-1]):
        refs[-1][i * rows : (i + 1) * rows, :] = ref[...]


def join(pieces):
    rows, width = pieces[0].shape
    return pl.pallas_call(
        join_body,
        out_shape=VMEM((len(pieces) * rows, width), BF16),
        in_specs=[in_vmem()] * len(pieces),
        out_specs=in_vmem(),
        compiler_params=grant(4),
        cost_estimate=cost(2e8, 4 * len(pieces) * rows * width),
        name="join",
    )(*[near(piece) for piece in pieces])


def attend_body(run_rows, query_half, key_halves, begun, final, *refs):
    query_ref, own_ref = refs[:2]
    pieces = refs[2 : 2 + len(key_halves)]
    refs = refs[2 + len(key_halves) :]
    if begun:
        mixed_ref, top_ref, sum_ref = refs[:3]
        refs = refs[3:]
    if final:
        out_ref, kv_ref = refs
    else:
        mixed_out, top_out, sum_out, kv_ref = refs
    block_rows = run_rows + TAG_ROWS
    held = [
        (piece, row, half)
        for piece, half in zip(pieces, key_halves)
        for row in range(0, piece.shape[0], block_rows)
    ]
    kv_width = pieces[0].shape[1] // 2
    kv_heads = kv_width // HEAD
    group = query_ref.shape[1] // kv_width
    lanes = group * run_rows
    step = (1.0 / math.sqrt(HEAD)) * math.log2(math.e)
    query_rows = pl.ds(query_half * run_rows, run_rows)
    own_at = None if begun else next(i for i, (_, _, half) in enumerate(held) if half == query_half)

    own = own_ref[run_rows:block_rows, :HEAD].astype(F32)[:1, :]
    hidden = []
    for number, (piece, row, half) in enumerate(held):
        kv_ref[pl.ds(number * run_rows, run_rows), :] = piece[row : row + run_rows, :]
        if query_half == 1 and half == 0:
            hidden.append(None)
        elif number == own_at:
            key = lax.broadcasted_iota(jnp.int32, (run_rows, lanes), 0)
            query = lax.broadcasted_iota(jnp.int32, (run_rows, lanes), 1)
            query = query - sum((query >= h * run_rows).astype(jnp.int32) for h in range(1, group)) * run_rows
            hidden.append(jnp.where(key <= query, 0.0, HIDE))
        else:
            tag = piece[row + run_rows : row + block_rows, :HEAD].astype(F32)[:1, :]
            seen = tag < own if half == 0 else tag > own
            line = jnp.where(seen, 0.0, HIDE)
            hidden.append(jnp.concatenate([line] * -(-lanes // HEAD), axis=1)[:, :lanes])

    for kv_head in range(kv_heads):
        keys = kv_ref[:, kv_head * HEAD : (kv_head + 1) * HEAD]
        values = kv_ref[:, kv_width + kv_head * HEAD : kv_width + (kv_head + 1) * HEAD]
        heads = [kv_head * group + i for i in range(group)]
        query = jnp.concatenate([query_ref[query_rows, h * HEAD : (h + 1) * HEAD] for h in heads], axis=0)
        scores = lax.dot_general(keys, query, (((1,), (1,)), ((), ())), preferred_element_type=F32)
        parts = []
        for number in range(len(held)):
            part = scores[number * run_rows : (number + 1) * run_rows] * step
            parts.append(part if hidden[number] is None else part + hidden[number])
        top = functools.reduce(jnp.maximum, [jnp.max(part, axis=0, keepdims=True) for part in parts])
        if begun:
            top = jnp.maximum(top, top_ref[kv_head])
        parts = [jnp.exp2(part - top) for part in parts]
        amount = sum(jnp.sum(part, axis=0, keepdims=True) for part in parts)
        weights = jnp.concatenate([part.astype(BF16) for part in parts], axis=0)
        mixed = lax.dot_general(values, weights, (((0,), (0,)), ((), ())), preferred_element_type=F32)
        rows = slice(kv_head * HEAD, (kv_head + 1) * HEAD)
        if begun:
            factor = jnp.exp2(top_ref[kv_head] - top)
            mixed = mixed + mixed_ref[rows, :] * factor
            amount = amount + sum_ref[kv_head] * factor
        if final:
            mean = (mixed / amount).T.astype(BF16)
            for i, h in enumerate(heads):
                out_ref[:, h * HEAD : (h + 1) * HEAD] = mean[i * run_rows : (i + 1) * run_rows, :]
        else:
            mixed_out[rows, :] = mixed
            top_out[kv_head] = top
            sum_out[kv_head] = amount


def attend(queries, query_half, own, piece_sets, begun=None, final=True):
    run_rows = queries.shape[0] // 2
    key_halves = [half for half, pieces in enumerate(piece_sets) for piece in pieces]
    pieces = [piece for pieces in piece_sets for piece in pieces]
    total = sum(piece.shape[0] for piece in pieces) // (run_rows + TAG_ROWS) * run_rows
    kv_width = pieces[0].shape[1] // 2
    width = queries.shape[1]
    lanes = width // kv_width * run_rows
    line = VMEM((kv_width // HEAD, 1, lanes), F32)
    state = (VMEM((kv_width, lanes), F32), line, line)
    operands = [queries, own, *pieces, *(begun or [])]
    return pl.pallas_call(
        functools.partial(attend_body, run_rows, query_half, key_halves, begun is not None, final),
        out_shape=VMEM((run_rows, width), BF16) if final else state,
        in_specs=[in_vmem()] * len(operands),
        out_specs=in_vmem() if final else (in_vmem(),) * 3,
        scratch_shapes=[VMEM((total, 2 * kv_width), BF16)],
        compiler_params=grant(20),
        cost_estimate=cost(4 * run_rows * total * width, total * pieces[0].shape[1] * 2),
    )(*[near(operand) for operand in operands])


def project_body(cores, blocks, half, own, att_ref, weight_ref, *rest):
    outs = rest[2:] if own else rest
    width = outs[0].shape[1] // len(blocks)
    tp = lax.axis_index("tp")
    for i, yb in enumerate(blocks):
        block = yb * cores + ((tp % cores) ^ (0 if own else 1))
        start = pl.multiple_of(block * width, HEAD)
        total = jnp.dot(att_ref[...], weight_ref[:, pl.ds(start, width)], preferred_element_type=F32)
        columns = slice(i * width, (i + 1) * width)
        if own:
            arrived, residual = rest[0], rest[1]
            mine = jnp.where(tp // cores == yb, 1.0, 0.0).astype(F32)
            total = total.astype(BF16).astype(F32) + arrived[:, columns].astype(F32)
            rows = pl.ds(half * arrived.shape[0], arrived.shape[0])
            total = total + mine * residual[rows, :].astype(F32)
        total = total.astype(BF16)
        row = 0
        for out in outs:
            out[:, columns] = total[row : row + out.shape[0]]
            row += out.shape[0]


def project(cores, blocks, half, attended, weight, block_width, cuts=(1,), arrived=None, residual=None):
    rows, depth = attended.shape
    width = block_width * len(blocks)
    own = arrived is not None
    operands = [attended, weight] + ([arrived, residual] if own else [])
    result = pl.pallas_call(
        functools.partial(project_body, cores, blocks, half, own),
        out_shape=tuple(VMEM((rows * cut // sum(cuts), width), BF16) for cut in cuts),
        in_specs=[in_vmem()] * len(operands),
        out_specs=(in_vmem(),) * len(cuts),
        compiler_params=grant(8),
        cost_estimate=cost(2 * rows * depth * width, depth * width * 2),
        name="project_own" if own else "project_other",
    )(*[near(operand) for operand in operands])
    return result if own else result[0]


def finish_body(ny, cores, row, rows, places, count, last, *refs):
    blocks = ny * cores
    gains, refs = refs[:blocks], refs[blocks:]
    parts = refs[:count]
    line_ref = refs[count]
    quant_ref, line_out, stream_ref, quant_vmem, stream_vmem, line_vmem, sems = refs[-7:]
    width = parts[0].shape[1]
    tp = lax.axis_index("tp")
    y, core = tp // cores, tp % cores

    def part(yb, k):
        number, first = places[yb, k]
        return parts[number][first : first + rows, :].astype(F32)

    def gain(yb, k):
        chosen = gains[k][...]
        for distance in range(1, ny):
            chosen = jnp.where((y ^ yb) == distance, gains[distance * cores + k][...], chosen)
        return chosen

    stream = part(0, 0)
    for yb in range(1, ny):
        stream = jnp.where(y == yb, part(yb, 0), stream)
    stream_vmem[...] = stream.astype(BF16)
    copies = [pltpu.make_async_copy(stream_vmem, stream_ref.at[pl.ds(row, rows), :], sems.at[blocks])]
    copies[0].start()
    totals = {}
    for yb in range(ny):
        for k in range(cores):
            value = part(yb, k)
            totals[yb, k] = jnp.sum(value * value, axis=1, keepdims=True)
    square = jnp.zeros((rows, 1), F32)
    for yb in range(ny):
        for cb in range(cores):
            chosen = totals[yb, 0]
            for k in range(1, cores):
                chosen = jnp.where((core ^ k) == cb, totals[yb, k], chosen)
            square = square + chosen
    root = lax.rsqrt(square / (blocks * width) + 1e-05)
    peak = jnp.zeros((rows, 1), F32)
    for yb in range(ny):
        for k in range(cores):
            value = part(yb, k) * gain(yb, k)
            peak = jnp.maximum(peak, jnp.max(jnp.abs(value), axis=1, keepdims=True))
    peak = peak * root + 1e-06
    factor = root / peak
    lanes = line_ref.shape[-1]
    lane = lax.broadcasted_iota(jnp.int32, (rows, lanes), 1)
    here = lax.broadcasted_iota(jnp.int32, (rows, lanes), 0) + row == lane
    line = jnp.sum(jnp.where(here, peak, 0.0), axis=0, keepdims=True)
    if row:
        line = line + line_ref[...]
    if last:
        line_vmem[...] = line.reshape(line_vmem.shape)
        copies.append(pltpu.make_async_copy(line_vmem, line_out, sems.at[blocks + 1]))
        copies[-1].start()
    else:
        line_out[...] = line
    for yb in range(ny):
        for k in range(cores):
            value = part(yb, k) * gain(yb, k) * factor
            slot = yb * cores + k
            start = pl.multiple_of((yb * cores + (core ^ k)) * width, HEAD)
            quant_vmem[slot] = value.astype(BF16)
            target = quant_ref.at[pl.ds(row, rows), pl.ds(start, width)]
            copies.append(pltpu.make_async_copy(quant_vmem.at[slot], target, sems.at[slot]))
            copies[-1].start()
    for copy in copies:
        copy.wait()


def finish(ny, cores, row, rows, all_rows, gains, parts, places, earlier):
    width = parts[0].shape[1]
    blocks = ny * cores
    last = row + rows == all_rows
    operands = [near(operand) for operand in (*gains, *parts)]
    out_shape = (
        jax.ShapeDtypeStruct((all_rows, blocks * width), BF16),
        jax.ShapeDtypeStruct((all_rows,), F32) if last else VMEM((1, all_rows), F32),
        jax.ShapeDtypeStruct((all_rows, width), BF16),
    )
    aliases = {}
    if earlier is not None:
        aliases = {len(operands) + 1: 0, len(operands) + 2: 2}
        operands += [near(earlier[1]), earlier[0], earlier[2]]
    else:
        operands += [near(jnp.zeros((1, all_rows), F32))]
    n = 1 + blocks + len(parts)
    return pl.pallas_call(
        functools.partial(finish_body, ny, cores, row, rows, places, len(parts), last),
        out_shape=out_shape,
        in_specs=[in_vmem()] * n + [in_place()] * (len(operands) - n),
        out_specs=(in_place(), in_place() if last else in_vmem(), in_place()),
        scratch_shapes=[
            VMEM((blocks, rows, width), BF16),
            VMEM((rows, width), BF16),
            VMEM((all_rows,), F32),
            pltpu.SemaphoreType.DMA((blocks + 2,)),
        ],
        input_output_aliases=aliases,
        compiler_params=grant(8),
        cost_estimate=cost(2e9, 4 * rows * blocks * width),
    )(*operands)


def swap(size, count, stride, distance):
    def partner(index):
        digit = (index // stride) % size
        return index + ((digit ^ distance) - digit) * stride

    return [(index, partner(index)) for index in range(count)]


def tree_sum(terms):
    terms = [term.astype(F32) for term in terms]
    while len(terms) > 1:
        terms = [terms[i] + terms[i + 1] for i in range(0, len(terms), 2)]
    return terms[0].astype(BF16)


def on_device(sizes, queries, keys, values, positions, residual, norm_gain, out_weight):
    nz, nx, ny, cores = sizes
    n_seq, n_tp = nz * nx, ny * cores
    all_rows, block_width = residual.shape
    run_rows = all_rows // 2

    def move_z(array, k):
        return lax.ppermute(array, "seq", swap(nz, n_seq, nx, k))

    def move_x(array, k):
        return lax.ppermute(array, "seq", swap(nx, n_seq, 1, k))

    def move_y(array, k):
        return lax.ppermute(array, "tp", swap(ny, n_tp, cores, k))

    def move_core(array, k):
        return lax.ppermute(array, "tp", swap(cores, n_tp, 1, k))

    low, high = pack(positions, keys, values)
    low_pieces = [low] + [move_x(low, j) for j in range(1, nx)]

    distances = [nz - 1] + [k for k in (1, *range(nz - 2, 1, -1)) if k < nz - 1]
    column = {k: move_z(low, k) for k in distances}
    for k in distances:
        low_pieces += [column[k]] + [move_x(column[k], j) for j in range(1, nx)]

    high_line = [high] + [move_x(high, j) for j in range(1, nx)]
    high_line = join([after(high_line[0], column[distances[0]]), *high_line[1:]])
    step, high_pieces = nz // 2, [high_line]
    firsts = {k: move_z(high_line, k) for k in dict.fromkeys((step, 1)) if k}
    while step:
        for held in list(high_pieces):
            if held is high_line and step in firsts:
                high_pieces.append(firsts[step])
            else:
                high_pieces.append(move_z(held, step))
        step //= 2

    begun = attend(queries, 0, low, [low_pieces[:-nx]], None, False)
    early = attend(queries, 0, low, [low_pieces[-nx:]], begun)
    sent, parts = [], []
    for yb in range(ny):
        other = project(cores, [yb], 0, early, out_weight, block_width)
        sent.append(move_core(other, 1))
    for yb in range(ny):
        own = project(cores, [yb], 0, early, out_weight, block_width, (1,), sent[yb], residual)[0]
        total = tree_sum([own] + [move_y(own, k) for k in range(1, ny)])
        parts += [total, move_core(total, 1)]
    gains = [norm_gain] + [move_y(norm_gain, k) for k in range(1, ny)]
    gains = [gain if j == 0 else move_core(gain, j) for gain in gains for j in range(cores)]
    places = {(yb, k): (yb * cores + k, 0) for yb in range(ny) for k in range(cores)}
    result = finish(ny, cores, 0, run_rows, all_rows, gains, parts, places, None)

    begun = attend(queries, 1, low, [low_pieces, high_pieces[:-1]], None, False)
    late = attend(queries, 1, low, [[], high_pieces[-1:]], begun)
    sent, parts = [], []
    for yb in range(ny):
        other = project(cores, [yb], 1, late, out_weight, block_width)
        sent.append(move_core(other, 1))
    for yb in range(ny):
        cuts = CUTS if yb == ny - 1 else (1,)
        owns = project(cores, [yb], 1, late, out_weight, block_width, cuts, sent[yb], residual)
        for own in owns:
            total = tree_sum([own] + [move_y(own, k) for k in range(1, ny)])
            parts += [total, move_core(total, 1)]
    row, blocks = 0, (ny - 1) * cores
    for i, share in enumerate(CUTS):
        rows = run_rows * share // sum(CUTS)
        places = {(yb, k): (yb * cores + k, row) for yb in range(ny - 1) for k in range(cores)}
        places.update({(ny - 1, k): (blocks + k, 0) for k in range(cores)})
        chosen = parts[:blocks] + parts[blocks + i * cores : blocks + (i + 1) * cores]
        result = finish(ny, cores, run_rows + row, rows, all_rows, gains, chosen, places, result)
        row += rows
    quantized, scale, stream = result
    return (quantized, scale, stream)


def sizes_of(mesh):
    along_seq, along_tp = list(mesh.devices[:, 0]), list(mesh.devices[0, :])
    nx = len({device.coords[0] for device in along_seq})
    ny = len({device.coords[1] for device in along_tp})
    return (len(along_seq) // nx, nx, ny, len(along_tp) // ny)


def solution(mesh):
    return jax.shard_map(
        functools.partial(on_device, sizes_of(mesh)),
        mesh=mesh,
        in_specs=(
            P("seq", "tp"),
            P("seq", "tp"),
            P("seq", "tp"),
            P("seq"),
            P("seq", "tp"),
            P(None, "tp"),
            P("tp", None),
        ),
        out_specs=(P("seq", None), P("seq"), P("seq", "tp")),
        check_vma=False,
    )
```

```python
import functools
import math

import jax
import jax.numpy as jnp
from jax import lax
from jax.experimental import pallas as pl
from jax.experimental.pallas import tpu as pltpu
from jax.sharding import PartitionSpec as P


HEAD = 128
TAG_ROWS = 8
HIDE = -1e30
CUTS = (1, 1)
VMEM = pltpu.VMEM
F32 = jnp.float32
BF16 = jnp.bfloat16


def in_vmem():
    return pl.BlockSpec(memory_space=VMEM)


def in_place():
    return pl.BlockSpec(memory_space=pl.ANY)


def near(array):
    return pltpu.with_memory_space_constraint(array, VMEM)


def far(array):
    return pltpu.with_memory_space_constraint(array, pltpu.HBM)


def after(array, *others):
    return lax.optimization_barrier((array, *others))[0]


def cost(flops, moved):
    return pl.CostEstimate(flops=int(flops), bytes_accessed=int(moved), transcendentals=0)


def grant(mib):
    return pltpu.CompilerParams(vmem_limit_bytes=mib << 20)


def pack_body(run_rows, pos_ref, key_ref, value_ref, low_ref, high_ref, number_ref, sems):
    width = key_ref.shape[1]
    copies = [pltpu.make_async_copy(pos_ref, number_ref, sems.at[4])]
    for half, out in enumerate((low_ref, high_ref)):
        rows = pl.ds(half * run_rows, run_rows)
        for i, ref in enumerate((key_ref, value_ref)):
            target = out.at[pl.ds(0, run_rows), pl.ds(i * width, width)]
            copies.append(pltpu.make_async_copy(ref.at[rows, :], target, sems.at[2 * half + i]))
    for copy in copies:
        copy.start()
    copies[0].wait()
    run = (number_ref[0] // run_rows).astype(F32)
    for out in (low_ref, high_ref):
        out[run_rows:, :] = jnp.full((TAG_ROWS, 2 * width), run, F32).astype(BF16)
    for copy in copies[1:]:
        copy.wait()


def pack(positions, keys, values):
    run_rows = keys.shape[0] // 2
    shape = (run_rows + TAG_ROWS, 2 * keys.shape[1])
    return pl.pallas_call(
        functools.partial(pack_body, run_rows),
        out_shape=(VMEM(shape, BF16), VMEM(shape, BF16)),
        in_specs=[in_place()] * 3,
        out_specs=(in_vmem(), in_vmem()),
        scratch_shapes=[pltpu.SMEM(positions.shape, jnp.int32), pltpu.SemaphoreType.DMA((5,))],
        compiler_params=grant(4),
        cost_estimate=cost(4e10, 4 * keys.size * 2),
        name="pack",
    )(far(positions), far(keys), far(values))


def join_body(*refs):
    rows = refs[0].shape[0]
    for i, ref in enumerate(refs[:-1]):
        refs[-1][i * rows : (i + 1) * rows, :] = ref[...]


def join(pieces):
    rows, width = pieces[0].shape
    return pl.pallas_call(
        join_body,
        out_shape=VMEM((len(pieces) * rows, width), BF16),
        in_specs=[in_vmem()] * len(pieces),
        out_specs=in_vmem(),
        compiler_params=grant(4),
        cost_estimate=cost(2e8, 4 * len(pieces) * rows * width),
        name="join",
    )(*[near(piece) for piece in pieces])


def attend_body(run_rows, query_half, key_halves, begun, final, *refs):
    query_ref, own_ref = refs[:2]
    pieces = refs[2 : 2 + len(key_halves)]
    refs = refs[2 + len(key_halves) :]
    if begun:
        mixed_ref, top_ref, sum_ref = refs[:3]
        refs = refs[3:]
    if final:
        out_ref, kv_ref = refs
    else:
        mixed_out, top_out, sum_out, kv_ref = refs
    block_rows = run_rows + TAG_ROWS
    held = [
        (piece, row, half)
        for piece, half in zip(pieces, key_halves)
        for row in range(0, piece.shape[0], block_rows)
    ]
    kv_width = pieces[0].shape[1] // 2
    kv_heads = kv_width // HEAD
    group = query_ref.shape[1] // kv_width
    lanes = group * run_rows
    step = (1.0 / math.sqrt(HEAD)) * math.log2(math.e)
    query_rows = pl.ds(query_half * run_rows, run_rows)
    own_at = None if begun else next(i for i, (_, _, half) in enumerate(held) if half == query_half)

    own = own_ref[run_rows:block_rows, :HEAD].astype(F32)[:1, :]
    hidden = []
    for number, (piece, row, half) in enumerate(held):
        kv_ref[pl.ds(number * run_rows, run_rows), :] = piece[row : row + run_rows, :]
        if query_half == 1 and half == 0:
            hidden.append(None)
        elif number == own_at:
            key = lax.broadcasted_iota(jnp.int32, (run_rows, lanes), 0)
            query = lax.broadcasted_iota(jnp.int32, (run_rows, lanes), 1)
            query = query - sum((query >= h * run_rows).astype(jnp.int32) for h in range(1, group)) * run_rows
            hidden.append(jnp.where(key <= query, 0.0, HIDE))
        else:
            tag = piece[row + run_rows : row + block_rows, :HEAD].astype(F32)[:1, :]
            seen = tag < own if half == 0 else tag > own
            line = jnp.where(seen, 0.0, HIDE)
            hidden.append(jnp.concatenate([line] * -(-lanes // HEAD), axis=1)[:, :lanes])

    for kv_head in range(kv_heads):
        keys = kv_ref[:, kv_head * HEAD : (kv_head + 1) * HEAD]
        values = kv_ref[:, kv_width + kv_head * HEAD : kv_width + (kv_head + 1) * HEAD]
        heads = [kv_head * group + i for i in range(group)]
        query = jnp.concatenate([query_ref[query_rows, h * HEAD : (h + 1) * HEAD] for h in heads], axis=0)
        scores = lax.dot_general(keys, query, (((1,), (1,)), ((), ())), preferred_element_type=F32)
        parts = []
        for number in range(len(held)):
            part = scores[number * run_rows : (number + 1) * run_rows] * step
            parts.append(part if hidden[number] is None else part + hidden[number])
        top = functools.reduce(jnp.maximum, [jnp.max(part, axis=0, keepdims=True) for part in parts])
        if begun:
            top = jnp.maximum(top, top_ref[kv_head])
        parts = [jnp.exp2(part - top) for part in parts]
        amount = sum(jnp.sum(part, axis=0, keepdims=True) for part in parts)
        weights = jnp.concatenate([part.astype(BF16) for part in parts], axis=0)
        mixed = lax.dot_general(values, weights, (((0,), (0,)), ((), ())), preferred_element_type=F32)
        rows = slice(kv_head * HEAD, (kv_head + 1) * HEAD)
        if begun:
            factor = jnp.exp2(top_ref[kv_head] - top)
            mixed = mixed + mixed_ref[rows, :] * factor
            amount = amount + sum_ref[kv_head] * factor
        if final:
            mean = (mixed / amount).T.astype(BF16)
            for i, h in enumerate(heads):
                out_ref[:, h * HEAD : (h + 1) * HEAD] = mean[i * run_rows : (i + 1) * run_rows, :]
        else:
            mixed_out[rows, :] = mixed
            top_out[kv_head] = top
            sum_out[kv_head] = amount


def attend(queries, query_half, own, piece_sets, begun=None, final=True):
    run_rows = queries.shape[0] // 2
    key_halves = [half for half, pieces in enumerate(piece_sets) for piece in pieces]
    pieces = [piece for pieces in piece_sets for piece in pieces]
    total = sum(piece.shape[0] for piece in pieces) // (run_rows + TAG_ROWS) * run_rows
    kv_width = pieces[0].shape[1] // 2
    width = queries.shape[1]
    lanes = width // kv_width * run_rows
    line = VMEM((kv_width // HEAD, 1, lanes), F32)
    state = (VMEM((kv_width, lanes), F32), line, line)
    operands = [queries, own, *pieces, *(begun or [])]
    return pl.pallas_call(
        functools.partial(attend_body, run_rows, query_half, key_halves, begun is not None, final),
        out_shape=VMEM((run_rows, width), BF16) if final else state,
        in_specs=[in_vmem()] * len(operands),
        out_specs=in_vmem() if final else (in_vmem(),) * 3,
        scratch_shapes=[VMEM((total, 2 * kv_width), BF16)],
        compiler_params=grant(20),
        cost_estimate=cost(4 * run_rows * total * width, total * pieces[0].shape[1] * 2),
    )(*[near(operand) for operand in operands])


def project_body(cores, blocks, half, distance, own, att_ref, weight_ref, *rest):
    outs = rest[2:] if own else rest
    width = outs[0].shape[1] // len(blocks)
    tp = lax.axis_index("tp")
    for i, yb in enumerate(blocks):
        block = yb * cores + ((tp % cores) ^ distance)
        start = pl.multiple_of(block * width, HEAD)
        total = jnp.dot(att_ref[...], weight_ref[:, pl.ds(start, width)], preferred_element_type=F32)
        columns = slice(i * width, (i + 1) * width)
        if own:
            arrived, residual = rest[0], rest[1]
            mine = jnp.where(tp // cores == yb, 1.0, 0.0).astype(F32)
            total = total.astype(BF16).astype(F32) + arrived[:, columns].astype(F32)
            rows = pl.ds(half * arrived.shape[0], arrived.shape[0])
            total = total + mine * residual[rows, :].astype(F32)
        total = total.astype(BF16)
        row = 0
        for out in outs:
            out[:, columns] = total[row : row + out.shape[0]]
            row += out.shape[0]


def project(cores, blocks, half, distance, attended, weight, block_width, cuts=(1,), arrived=None, residual=None):
    rows, depth = attended.shape
    width = block_width * len(blocks)
    own = arrived is not None
    operands = [attended, weight] + ([arrived, residual] if own else [])
    result = pl.pallas_call(
        functools.partial(project_body, cores, blocks, half, distance, own),
        out_shape=tuple(VMEM((rows * cut // sum(cuts), width), BF16) for cut in cuts),
        in_specs=[in_vmem()] * len(operands),
        out_specs=(in_vmem(),) * len(cuts),
        compiler_params=grant(8),
        cost_estimate=cost(2 * rows * depth * width, depth * width * 2),
        name="project_own" if own else "project_other",
    )(*[near(operand) for operand in operands])
    return result if own else result[0]


def combine_body(cores, yb, half, own_ref, arrived_ref, residual_ref, out_ref):
    rows = own_ref.shape[0]
    mine = jnp.where(lax.axis_index("tp") // cores == yb, 1.0, 0.0).astype(F32)
    total = own_ref[...].astype(F32) + arrived_ref[...].astype(F32)
    total = total + mine * residual_ref[half * rows : (half + 1) * rows, :].astype(F32)
    out_ref[...] = total.astype(BF16)


def combine(cores, yb, half, own, arrived, residual):
    return pl.pallas_call(
        functools.partial(combine_body, cores, yb, half),
        out_shape=VMEM(own.shape, BF16),
        in_specs=[in_vmem()] * 3,
        out_specs=in_vmem(),
        compiler_params=grant(8),
        cost_estimate=cost(2e8, 8 * own.size),
        name="combine",
    )(near(own), near(arrived), near(residual))


def finish_body(ny, cores, row, rows, places, count, last, *refs):
    blocks = ny * cores
    gains, refs = refs[:blocks], refs[blocks:]
    parts = refs[:count]
    line_ref = refs[count]
    quant_ref, line_out, stream_ref, quant_vmem, stream_vmem, line_vmem, sems = refs[-7:]
    width = parts[0].shape[1]
    tp = lax.axis_index("tp")
    y, core = tp // cores, tp % cores

    def part(yb, k):
        number, first = places[yb, k]
        return parts[number][first : first + rows, :].astype(F32)

    def gain(yb, k):
        chosen = gains[k][...]
        for distance in range(1, ny):
            chosen = jnp.where((y ^ yb) == distance, gains[distance * cores + k][...], chosen)
        return chosen

    stream = part(0, 0)
    for yb in range(1, ny):
        stream = jnp.where(y == yb, part(yb, 0), stream)
    stream_vmem[...] = stream.astype(BF16)
    copies = [pltpu.make_async_copy(stream_vmem, stream_ref.at[pl.ds(row, rows), :], sems.at[blocks])]
    copies[0].start()
    totals = {}
    for yb in range(ny):
        for k in range(cores):
            value = part(yb, k)
            totals[yb, k] = jnp.sum(value * value, axis=1, keepdims=True)
    square = jnp.zeros((rows, 1), F32)
    for yb in range(ny):
        for cb in range(cores):
            chosen = totals[yb, 0]
            for k in range(1, cores):
                chosen = jnp.where((core ^ k) == cb, totals[yb, k], chosen)
            square = square + chosen
    root = lax.rsqrt(square / (blocks * width) + 1e-05)
    peak = jnp.zeros((rows, 1), F32)
    for yb in range(ny):
        for k in range(cores):
            value = part(yb, k) * gain(yb, k)
            peak = jnp.maximum(peak, jnp.max(jnp.abs(value), axis=1, keepdims=True))
    peak = peak * root + 1e-06
    factor = root / peak
    lanes = line_ref.shape[-1]
    lane = lax.broadcasted_iota(jnp.int32, (rows, lanes), 1)
    here = lax.broadcasted_iota(jnp.int32, (rows, lanes), 0) + row == lane
    line = jnp.sum(jnp.where(here, peak, 0.0), axis=0, keepdims=True)
    if row:
        line = line + line_ref[...]
    if last:
        line_vmem[...] = line.reshape(line_vmem.shape)
        copies.append(pltpu.make_async_copy(line_vmem, line_out, sems.at[blocks + 1]))
        copies[-1].start()
    else:
        line_out[...] = line
    for yb in range(ny):
        for k in range(cores):
            value = part(yb, k) * gain(yb, k) * factor
            slot = yb * cores + k
            start = pl.multiple_of((yb * cores + (core ^ k)) * width, HEAD)
            quant_vmem[slot] = value.astype(BF16)
            target = quant_ref.at[pl.ds(row, rows), pl.ds(start, width)]
            copies.append(pltpu.make_async_copy(quant_vmem.at[slot], target, sems.at[slot]))
            copies[-1].start()
    for copy in copies:
        copy.wait()


def finish(ny, cores, row, rows, all_rows, gains, parts, places, earlier):
    width = parts[0].shape[1]
    blocks = ny * cores
    last = row + rows == all_rows
    operands = [near(operand) for operand in (*gains, *parts)]
    out_shape = (
        jax.ShapeDtypeStruct((all_rows, blocks * width), BF16),
        jax.ShapeDtypeStruct((all_rows,), F32) if last else VMEM((1, all_rows), F32),
        jax.ShapeDtypeStruct((all_rows, width), BF16),
    )
    aliases = {}
    if earlier is not None:
        aliases = {len(operands) + 1: 0, len(operands) + 2: 2}
        operands += [near(earlier[1]), earlier[0], earlier[2]]
    else:
        operands += [near(jnp.zeros((1, all_rows), F32))]
    n = 1 + blocks + len(parts)
    return pl.pallas_call(
        functools.partial(finish_body, ny, cores, row, rows, places, len(parts), last),
        out_shape=out_shape,
        in_specs=[in_vmem()] * n + [in_place()] * (len(operands) - n),
        out_specs=(in_place(), in_place() if last else in_vmem(), in_place()),
        scratch_shapes=[
            VMEM((blocks, rows, width), BF16),
            VMEM((rows, width), BF16),
            VMEM((all_rows,), F32),
            pltpu.SemaphoreType.DMA((blocks + 2,)),
        ],
        input_output_aliases=aliases,
        compiler_params=grant(8),
        cost_estimate=cost(2e9, 4 * rows * blocks * width),
    )(*operands)


def swap(size, count, stride, distance):
    def partner(index):
        digit = (index // stride) % size
        return index + ((digit ^ distance) - digit) * stride

    return [(index, partner(index)) for index in range(count)]


def tree_sum(terms):
    terms = [term.astype(F32) for term in terms]
    while len(terms) > 1:
        terms = [terms[i] + terms[i + 1] for i in range(0, len(terms), 2)]
    return terms[0].astype(BF16)


def on_device(sizes, queries, keys, values, positions, residual, norm_gain, out_weight):
    nz, nx, ny, cores = sizes
    n_seq, n_tp = nz * nx, ny * cores
    all_rows, block_width = residual.shape
    run_rows = all_rows // 2

    def move_z(array, k):
        return lax.ppermute(array, "seq", swap(nz, n_seq, nx, k))

    def move_x(array, k):
        return lax.ppermute(array, "seq", swap(nx, n_seq, 1, k))

    def move_y(array, k):
        return lax.ppermute(array, "tp", swap(ny, n_tp, cores, k))

    def move_core(array, k):
        return lax.ppermute(array, "tp", swap(cores, n_tp, 1, k))

    low, high = pack(positions, keys, values)
    low_pieces = [low] + [move_x(low, j) for j in range(1, nx)]

    distances = [nz - 1] + [k for k in (1, *range(nz - 2, 1, -1)) if k < nz - 1]
    column = {k: move_z(low, k) for k in distances}
    for k in distances:
        low_pieces += [column[k]] + [move_x(column[k], j) for j in range(1, nx)]

    high_line = [high] + [move_x(high, j) for j in range(1, nx)]
    high_line = join([after(high_line[0], column[distances[0]]), *high_line[1:]])
    step, high_pieces = nz // 2, [high_line]
    firsts = {k: move_z(high_line, k) for k in dict.fromkeys((step, 1)) if k}
    while step:
        for held in list(high_pieces):
            if held is high_line and step in firsts:
                high_pieces.append(firsts[step])
            else:
                high_pieces.append(move_z(held, step))
        step //= 2

    begun = attend(queries, 0, low, [low_pieces[:-nx]], None, False)
    early = attend(queries, 0, low, [low_pieces[-nx:]], begun)
    parts = []
    for yb in range(ny):
        other = project(cores, [yb], 0, 1, early, out_weight, block_width)
        arrived = move_core(other, 1)
        if yb == 0:
            own = project(cores, [yb], 0, 0, early, out_weight, block_width)
        else:
            own = project(cores, [yb], 0, 0, early, out_weight, block_width, (1,), arrived, residual)[0]
        if yb == 0:
            own = combine(cores, yb, 0, own, arrived, residual)
        total = tree_sum([own] + [move_y(own, k) for k in range(1, ny)])
        parts += [total, move_core(total, 1)]
    gains = [norm_gain] + [move_y(norm_gain, k) for k in range(1, ny)]
    gains = [gain if j == 0 else move_core(gain, j) for gain in gains for j in range(cores)]
    places = {(yb, k): (yb * cores + k, 0) for yb in range(ny) for k in range(cores)}
    result = finish(ny, cores, 0, run_rows, all_rows, gains, parts, places, None)

    begun = attend(queries, 1, low, [low_pieces, high_pieces[:-1]], None, False)
    late = attend(queries, 1, low, [[], high_pieces[-1:]], begun)
    parts = []
    for yb in range(ny):
        cuts = CUTS if yb == ny - 1 else (1,)
        other = project(cores, [yb], 1, 1, late, out_weight, block_width)
        arrived = move_core(other, 1)
        if yb == 0 and yb < ny - 1:
            own = project(cores, [yb], 1, 0, late, out_weight, block_width)
        else:
            owns = project(cores, [yb], 1, 0, late, out_weight, block_width, cuts, arrived, residual)
        if yb == 0 and yb < ny - 1:
            owns = [combine(cores, yb, 1, own, arrived, residual)]
        for own in owns:
            total = tree_sum([own] + [move_y(own, k) for k in range(1, ny)])
            parts += [total, move_core(total, 1)]
    row, blocks = 0, (ny - 1) * cores
    for i, share in enumerate(CUTS):
        rows = run_rows * share // sum(CUTS)
        places = {(yb, k): (yb * cores + k, row) for yb in range(ny - 1) for k in range(cores)}
        places.update({(ny - 1, k): (blocks + k, 0) for k in range(cores)})
        chosen = parts[:blocks] + parts[blocks + i * cores : blocks + (i + 1) * cores]
        result = finish(ny, cores, run_rows + row, rows, all_rows, gains, chosen, places, result)
        row += rows
    quantized, scale, stream = result
    return (quantized, scale, stream)


def sizes_of(mesh):
    along_seq, along_tp = list(mesh.devices[:, 0]), list(mesh.devices[0, :])
    nx = len({device.coords[0] for device in along_seq})
    ny = len({device.coords[1] for device in along_tp})
    return (len(along_seq) // nx, nx, ny, len(along_tp) // ny)


def solution(mesh):
    return jax.shard_map(
        functools.partial(on_device, sizes_of(mesh)),
        mesh=mesh,
        in_specs=(
            P("seq", "tp"),
            P("seq", "tp"),
            P("seq", "tp"),
            P("seq"),
            P("seq", "tp"),
            P(None, "tp"),
            P("tp", None),
        ),
        out_specs=(P("seq", None), P("seq"), P("seq", "tp")),
        check_vma=False,
    )
```

```python
import functools
import math

import jax
import jax.numpy as jnp
from jax import lax
from jax.experimental import pallas as pl
from jax.experimental.pallas import tpu as pltpu
from jax.sharding import PartitionSpec as P


HEAD = 128
TAG_ROWS = 8
HIDE = -1e30
CUTS = (1, 1)
VMEM = pltpu.VMEM
F32 = jnp.float32
BF16 = jnp.bfloat16


def in_vmem():
    return pl.BlockSpec(memory_space=VMEM)


def in_place():
    return pl.BlockSpec(memory_space=pl.ANY)


def near(array):
    return pltpu.with_memory_space_constraint(array, VMEM)


def far(array):
    return pltpu.with_memory_space_constraint(array, pltpu.HBM)


def after(array, *others):
    return lax.optimization_barrier((array, *others))[0]


def cost(flops, moved):
    return pl.CostEstimate(flops=int(flops), bytes_accessed=int(moved), transcendentals=0)


def grant(mib):
    return pltpu.CompilerParams(vmem_limit_bytes=mib << 20)


def pack_body(run_rows, pos_ref, key_ref, value_ref, low_ref, high_ref, number_ref, sems):
    width = key_ref.shape[1]
    copies = [pltpu.make_async_copy(pos_ref, number_ref, sems.at[4])]
    for half, out in enumerate((low_ref, high_ref)):
        rows = pl.ds(half * run_rows, run_rows)
        for i, ref in enumerate((key_ref, value_ref)):
            target = out.at[pl.ds(0, run_rows), pl.ds(i * width, width)]
            copies.append(pltpu.make_async_copy(ref.at[rows, :], target, sems.at[2 * half + i]))
    for copy in copies:
        copy.start()
    copies[0].wait()
    run = (number_ref[0] // run_rows).astype(F32)
    for out in (low_ref, high_ref):
        out[run_rows:, :] = jnp.full((TAG_ROWS, 2 * width), run, F32).astype(BF16)
    for copy in copies[1:]:
        copy.wait()


def pack(positions, keys, values):
    run_rows = keys.shape[0] // 2
    shape = (run_rows + TAG_ROWS, 2 * keys.shape[1])
    return pl.pallas_call(
        functools.partial(pack_body, run_rows),
        out_shape=(VMEM(shape, BF16), VMEM(shape, BF16)),
        in_specs=[in_place()] * 3,
        out_specs=(in_vmem(), in_vmem()),
        scratch_shapes=[pltpu.SMEM(positions.shape, jnp.int32), pltpu.SemaphoreType.DMA((5,))],
        compiler_params=grant(4),
        cost_estimate=cost(4e10, 4 * keys.size * 2),
        name="pack",
    )(far(positions), far(keys), far(values))


def join_body(*refs):
    rows = refs[0].shape[0]
    for i, ref in enumerate(refs[:-1]):
        refs[-1][i * rows : (i + 1) * rows, :] = ref[...]


def join(pieces):
    rows, width = pieces[0].shape
    return pl.pallas_call(
        join_body,
        out_shape=VMEM((len(pieces) * rows, width), BF16),
        in_specs=[in_vmem()] * len(pieces),
        out_specs=in_vmem(),
        compiler_params=grant(4),
        cost_estimate=cost(2e8, 4 * len(pieces) * rows * width),
        name="join",
    )(*[near(piece) for piece in pieces])


def attend_body(run_rows, query_half, key_halves, begun, final, *refs):
    query_ref, own_ref = refs[:2]
    pieces = refs[2 : 2 + len(key_halves)]
    refs = refs[2 + len(key_halves) :]
    if begun:
        mixed_ref, top_ref, sum_ref = refs[:3]
        refs = refs[3:]
    if final:
        out_ref, kv_ref = refs
    else:
        mixed_out, top_out, sum_out, kv_ref = refs
    block_rows = run_rows + TAG_ROWS
    held = [
        (piece, row, half)
        for piece, half in zip(pieces, key_halves)
        for row in range(0, piece.shape[0], block_rows)
    ]
    kv_width = pieces[0].shape[1] // 2
    kv_heads = kv_width // HEAD
    group = query_ref.shape[1] // kv_width
    lanes = group * run_rows
    step = (1.0 / math.sqrt(HEAD)) * math.log2(math.e)
    query_rows = pl.ds(query_half * run_rows, run_rows)
    own_at = None if begun else next(i for i, (_, _, half) in enumerate(held) if half == query_half)

    own = own_ref[run_rows:block_rows, :HEAD].astype(F32)[:1, :]
    hidden = []
    for number, (piece, row, half) in enumerate(held):
        kv_ref[pl.ds(number * run_rows, run_rows), :] = piece[row : row + run_rows, :]
        if query_half == 1 and half == 0:
            hidden.append(None)
        elif number == own_at:
            key = lax.broadcasted_iota(jnp.int32, (run_rows, lanes), 0)
            query = lax.broadcasted_iota(jnp.int32, (run_rows, lanes), 1)
            query = query - sum((query >= h * run_rows).astype(jnp.int32) for h in range(1, group)) * run_rows
            hidden.append(jnp.where(key <= query, 0.0, HIDE))
        else:
            tag = piece[row + run_rows : row + block_rows, :HEAD].astype(F32)[:1, :]
            seen = tag < own if half == 0 else tag > own
            line = jnp.where(seen, 0.0, HIDE)
            hidden.append(jnp.concatenate([line] * -(-lanes // HEAD), axis=1)[:, :lanes])

    for kv_head in range(kv_heads):
        keys = kv_ref[:, kv_head * HEAD : (kv_head + 1) * HEAD]
        values = kv_ref[:, kv_width + kv_head * HEAD : kv_width + (kv_head + 1) * HEAD]
        heads = [kv_head * group + i for i in range(group)]
        query = jnp.concatenate([query_ref[query_rows, h * HEAD : (h + 1) * HEAD] for h in heads], axis=0)
        scores = lax.dot_general(keys, query, (((1,), (1,)), ((), ())), preferred_element_type=F32)
        parts = []
        for number in range(len(held)):
            part = scores[number * run_rows : (number + 1) * run_rows] * step
            parts.append(part if hidden[number] is None else part + hidden[number])
        top = functools.reduce(jnp.maximum, [jnp.max(part, axis=0, keepdims=True) for part in parts])
        if begun:
            top = jnp.maximum(top, top_ref[kv_head])
        parts = [jnp.exp2(part - top) for part in parts]
        amount = sum(jnp.sum(part, axis=0, keepdims=True) for part in parts)
        weights = jnp.concatenate([part.astype(BF16) for part in parts], axis=0)
        mixed = lax.dot_general(values, weights, (((0,), (0,)), ((), ())), preferred_element_type=F32)
        rows = slice(kv_head * HEAD, (kv_head + 1) * HEAD)
        if begun:
            factor = jnp.exp2(top_ref[kv_head] - top)
            mixed = mixed + mixed_ref[rows, :] * factor
            amount = amount + sum_ref[kv_head] * factor
        if final:
            mean = (mixed / amount).T.astype(BF16)
            for i, h in enumerate(heads):
                out_ref[:, h * HEAD : (h + 1) * HEAD] = mean[i * run_rows : (i + 1) * run_rows, :]
        else:
            mixed_out[rows, :] = mixed
            top_out[kv_head] = top
            sum_out[kv_head] = amount


def attend(queries, query_half, own, piece_sets, begun=None, final=True):
    run_rows = queries.shape[0] // 2
    key_halves = [half for half, pieces in enumerate(piece_sets) for piece in pieces]
    pieces = [piece for pieces in piece_sets for piece in pieces]
    total = sum(piece.shape[0] for piece in pieces) // (run_rows + TAG_ROWS) * run_rows
    kv_width = pieces[0].shape[1] // 2
    width = queries.shape[1]
    lanes = width // kv_width * run_rows
    line = VMEM((kv_width // HEAD, 1, lanes), F32)
    state = (VMEM((kv_width, lanes), F32), line, line)
    operands = [queries, own, *pieces, *(begun or [])]
    return pl.pallas_call(
        functools.partial(attend_body, run_rows, query_half, key_halves, begun is not None, final),
        out_shape=VMEM((run_rows, width), BF16) if final else state,
        in_specs=[in_vmem()] * len(operands),
        out_specs=in_vmem() if final else (in_vmem(),) * 3,
        scratch_shapes=[VMEM((total, 2 * kv_width), BF16)],
        compiler_params=grant(20),
        cost_estimate=cost(4 * run_rows * total * width, total * pieces[0].shape[1] * 2),
        name="attend",
    )(*[near(operand) for operand in operands])


def project_body(cores, blocks, half, distance, own, att_ref, weight_ref, *rest):
    outs = rest[2:] if own else rest
    width = outs[0].shape[1] // len(blocks)
    tp = lax.axis_index("tp")
    for i, yb in enumerate(blocks):
        block = yb * cores + ((tp % cores) ^ distance)
        start = pl.multiple_of(block * width, HEAD)
        total = jnp.dot(att_ref[...], weight_ref[:, pl.ds(start, width)], preferred_element_type=F32)
        columns = slice(i * width, (i + 1) * width)
        if own:
            arrived, residual = rest[0], rest[1]
            mine = jnp.where(tp // cores == yb, 1.0, 0.0).astype(F32)
            total = total.astype(BF16).astype(F32) + arrived[:, columns].astype(F32)
            rows = pl.ds(half * arrived.shape[0], arrived.shape[0])
            total = total + mine * residual[rows, :].astype(F32)
        total = total.astype(BF16)
        row = 0
        for out in outs:
            out[:, columns] = total[row : row + out.shape[0]]
            row += out.shape[0]


def project(cores, blocks, half, distance, attended, weight, block_width, cuts=(1,), arrived=None, residual=None):
    rows, depth = attended.shape
    width = block_width * len(blocks)
    own = arrived is not None
    operands = [attended, weight] + ([arrived, residual] if own else [])
    result = pl.pallas_call(
        functools.partial(project_body, cores, blocks, half, distance, own),
        out_shape=tuple(VMEM((rows * cut // sum(cuts), width), BF16) for cut in cuts),
        in_specs=[in_vmem()] * len(operands),
        out_specs=(in_vmem(),) * len(cuts),
        compiler_params=grant(8),
        cost_estimate=cost(2 * rows * depth * width, depth * width * 2),
        name="project",
    )(*[near(operand) for operand in operands])
    return result if own else result[0]


def combine_body(cores, yb, half, own_ref, arrived_ref, residual_ref, out_ref):
    rows = own_ref.shape[0]
    mine = jnp.where(lax.axis_index("tp") // cores == yb, 1.0, 0.0).astype(F32)
    total = own_ref[...].astype(F32) + arrived_ref[...].astype(F32)
    total = total + mine * residual_ref[half * rows : (half + 1) * rows, :].astype(F32)
    out_ref[...] = total.astype(BF16)


def combine(cores, yb, half, own, arrived, residual):
    return pl.pallas_call(
        functools.partial(combine_body, cores, yb, half),
        out_shape=VMEM(own.shape, BF16),
        in_specs=[in_vmem()] * 3,
        out_specs=in_vmem(),
        compiler_params=grant(8),
        cost_estimate=cost(2e8, 8 * own.size),
        name="combine",
    )(near(own), near(arrived), near(residual))


def finish_body(ny, cores, row, rows, places, count, last, *refs):
    blocks = ny * cores
    gains, refs = refs[:blocks], refs[blocks:]
    parts = refs[:count]
    line_ref = refs[count]
    quant_ref, line_out, stream_ref, quant_vmem, stream_vmem, line_vmem, sems = refs[-7:]
    width = parts[0].shape[1]
    tp = lax.axis_index("tp")
    y, core = tp // cores, tp % cores

    def part(yb, k):
        number, first = places[yb, k]
        return parts[number][first : first + rows, :].astype(F32)

    def gain(yb, k):
        chosen = gains[k][...]
        for distance in range(1, ny):
            chosen = jnp.where((y ^ yb) == distance, gains[distance * cores + k][...], chosen)
        return chosen

    stream = part(0, 0)
    for yb in range(1, ny):
        stream = jnp.where(y == yb, part(yb, 0), stream)
    stream_vmem[...] = stream.astype(BF16)
    copies = [pltpu.make_async_copy(stream_vmem, stream_ref.at[pl.ds(row, rows), :], sems.at[blocks])]
    copies[0].start()
    totals = {}
    for yb in range(ny):
        for k in range(cores):
            value = part(yb, k)
            totals[yb, k] = jnp.sum(value * value, axis=1, keepdims=True)
    square = jnp.zeros((rows, 1), F32)
    for yb in range(ny):
        for cb in range(cores):
            chosen = totals[yb, 0]
            for k in range(1, cores):
                chosen = jnp.where((core ^ k) == cb, totals[yb, k], chosen)
            square = square + chosen
    root = lax.rsqrt(square / (blocks * width) + 1e-05)
    peak = jnp.zeros((rows, 1), F32)
    for yb in range(ny):
        for k in range(cores):
            value = part(yb, k) * gain(yb, k)
            peak = jnp.maximum(peak, jnp.max(jnp.abs(value), axis=1, keepdims=True))
    peak = peak * root + 1e-06
    factor = root / peak
    lanes = line_ref.shape[-1]
    lane = lax.broadcasted_iota(jnp.int32, (rows, lanes), 1)
    here = lax.broadcasted_iota(jnp.int32, (rows, lanes), 0) + row == lane
    line = jnp.sum(jnp.where(here, peak, 0.0), axis=0, keepdims=True)
    if row:
        line = line + line_ref[...]
    if last:
        line_vmem[...] = line.reshape(line_vmem.shape)
        copies.append(pltpu.make_async_copy(line_vmem, line_out, sems.at[blocks + 1]))
        copies[-1].start()
    else:
        line_out[...] = line
    for yb in range(ny):
        for k in range(cores):
            value = part(yb, k) * gain(yb, k) * factor
            slot = yb * cores + k
            start = pl.multiple_of((yb * cores + (core ^ k)) * width, HEAD)
            quant_vmem[slot] = value.astype(BF16)
            target = quant_ref.at[pl.ds(row, rows), pl.ds(start, width)]
            copies.append(pltpu.make_async_copy(quant_vmem.at[slot], target, sems.at[slot]))
            copies[-1].start()
    for copy in copies:
        copy.wait()


def finish(ny, cores, row, rows, all_rows, gains, parts, places, earlier):
    width = parts[0].shape[1]
    blocks = ny * cores
    last = row + rows == all_rows
    operands = [near(operand) for operand in (*gains, *parts)]
    out_shape = (
        jax.ShapeDtypeStruct((all_rows, blocks * width), BF16),
        jax.ShapeDtypeStruct((all_rows,), F32) if last else VMEM((1, all_rows), F32),
        jax.ShapeDtypeStruct((all_rows, width), BF16),
    )
    aliases = {}
    if earlier is not None:
        aliases = {len(operands) + 1: 0, len(operands) + 2: 2}
        operands += [near(earlier[1]), earlier[0], earlier[2]]
    else:
        operands += [near(jnp.zeros((1, all_rows), F32))]
    n = 1 + blocks + len(parts)
    return pl.pallas_call(
        functools.partial(finish_body, ny, cores, row, rows, places, len(parts), last),
        out_shape=out_shape,
        in_specs=[in_vmem()] * n + [in_place()] * (len(operands) - n),
        out_specs=(in_place(), in_place() if last else in_vmem(), in_place()),
        scratch_shapes=[
            VMEM((blocks, rows, width), BF16),
            VMEM((rows, width), BF16),
            VMEM((all_rows,), F32),
            pltpu.SemaphoreType.DMA((blocks + 2,)),
        ],
        input_output_aliases=aliases,
        compiler_params=grant(8),
        cost_estimate=cost(2e9, 4 * rows * blocks * width),
        name="finish",
    )(*operands)


def swap(size, count, stride, distance):
    def partner(index):
        digit = (index // stride) % size
        return index + ((digit ^ distance) - digit) * stride

    return [(index, partner(index)) for index in range(count)]


def tree_sum(terms):
    terms = [term.astype(F32) for term in terms]
    while len(terms) > 1:
        terms = [terms[i] + terms[i + 1] for i in range(0, len(terms), 2)]
    return terms[0].astype(BF16)


def on_device(sizes, queries, keys, values, positions, residual, norm_gain, out_weight):
    nz, nx, ny, cores = sizes
    n_seq, n_tp = nz * nx, ny * cores
    all_rows, block_width = residual.shape
    run_rows = all_rows // 2

    def move_z(array, k):
        return lax.ppermute(array, "seq", swap(nz, n_seq, nx, k))

    def move_x(array, k):
        return lax.ppermute(array, "seq", swap(nx, n_seq, 1, k))

    def move_y(array, k):
        return lax.ppermute(array, "tp", swap(ny, n_tp, cores, k))

    def move_core(array, k):
        return lax.ppermute(array, "tp", swap(cores, n_tp, 1, k))

    low, high = pack(positions, keys, values)
    low_pieces = [low] + [move_x(low, j) for j in range(1, nx)]

    distances = [nz - 1] + [k for k in (1, *range(nz - 2, 1, -1)) if k < nz - 1]
    column = {k: move_z(low, k) for k in distances}
    for k in distances:
        low_pieces += [column[k]] + [move_x(column[k], j) for j in range(1, nx)]

    high_line = [high] + [move_x(high, j) for j in range(1, nx)]
    high_line = join([after(high_line[0], column[distances[0]]), *high_line[1:]])
    step, high_pieces = nz // 2, [high_line]
    firsts = {k: move_z(high_line, k) for k in dict.fromkeys((step, 1)) if k}
    while step:
        for held in list(high_pieces):
            if held is high_line and step in firsts:
                high_pieces.append(firsts[step])
            else:
                high_pieces.append(move_z(held, step))
        step //= 2

    begun = attend(queries, 0, low, [low_pieces[: nx + 1]], None, False)
    early = attend(queries, 0, low, [low_pieces[nx + 1 :]], begun)
    parts = []
    for yb in range(ny):
        other = project(cores, [yb], 0, 1, early, out_weight, block_width)
        arrived = move_core(other, 1)
        if yb == 0:
            own = project(cores, [yb], 0, 0, early, out_weight, block_width)
        else:
            own = project(cores, [yb], 0, 0, early, out_weight, block_width, (1,), arrived, residual)[0]
        if yb == 0:
            own = combine(cores, yb, 0, own, arrived, residual)
        total = tree_sum([own] + [move_y(own, k) for k in range(1, ny)])
        parts += [total, move_core(total, 1)]
    gains = [norm_gain] + [move_y(norm_gain, k) for k in range(1, ny)]
    gains = [gain if j == 0 else move_core(gain, j) for gain in gains for j in range(cores)]
    places = {(yb, k): (yb * cores + k, 0) for yb in range(ny) for k in range(cores)}
    result = finish(ny, cores, 0, run_rows, all_rows, gains, parts, places, None)

    begun = attend(queries, 1, low, [low_pieces, high_pieces[:-1]], None, False)
    late = attend(queries, 1, low, [[], high_pieces[-1:]], begun)
    parts = []
    for yb in range(ny):
        cuts = CUTS if yb == ny - 1 else (1,)
        other = project(cores, [yb], 1, 1, late, out_weight, block_width)
        arrived = move_core(other, 1)
        if yb == 0 and yb < ny - 1:
            own = project(cores, [yb], 1, 0, late, out_weight, block_width)
        else:
            owns = project(cores, [yb], 1, 0, late, out_weight, block_width, cuts, arrived, residual)
        if yb == 0 and yb < ny - 1:
            owns = [combine(cores, yb, 1, own, arrived, residual)]
        for own in owns:
            total = tree_sum([own] + [move_y(own, k) for k in range(1, ny)])
            parts += [total, move_core(total, 1)]
    row, blocks = 0, (ny - 1) * cores
    for i, share in enumerate(CUTS):
        rows = run_rows * share // sum(CUTS)
        places = {(yb, k): (yb * cores + k, row) for yb in range(ny - 1) for k in range(cores)}
        places.update({(ny - 1, k): (blocks + k, 0) for k in range(cores)})
        chosen = parts[:blocks] + parts[blocks + i * cores : blocks + (i + 1) * cores]
        result = finish(ny, cores, run_rows + row, rows, all_rows, gains, chosen, places, result)
        row += rows
    quantized, scale, stream = result
    return (quantized, scale, stream)


def sizes_of(mesh):
    along_seq, along_tp = list(mesh.devices[:, 0]), list(mesh.devices[0, :])
    nx = len({device.coords[0] for device in along_seq})
    ny = len({device.coords[1] for device in along_tp})
    return (len(along_seq) // nx, nx, ny, len(along_tp) // ny)


def solution(mesh):
    return jax.shard_map(
        functools.partial(on_device, sizes_of(mesh)),
        mesh=mesh,
        in_specs=(
            P("seq", "tp"),
            P("seq", "tp"),
            P("seq", "tp"),
            P("seq"),
            P("seq", "tp"),
            P(None, "tp"),
            P("tp", None),
        ),
        out_specs=(P("seq", None), P("seq"), P("seq", "tp")),
        check_vma=False,
    )
```
